32 devices in a mesh: row: 4 (over z), col: 8 (over y, x, core).
Axes of the slice: x: 2, y: 2, z: 4, core: 2. Of those that a mesh axis runs over, the one named last changes fastest.
Arguments:
- w_one: float32 [4, 8, 2, 256, 1024], P('row', 'col')
- w_two: float32 [4, 8, 2, 1024, 256], P('row', 'col')
- inputs: bfloat16 [4, 8, 3, 1024, 256], P('row', 'col')
- targets: bfloat16 [4, 8, 3, 1024, 256], P('row', 'col')
Outputs:
- output 1: float32 [4, 8, 2, 256, 1024], P('row', 'col')
- output 2: float32 [4, 8, 2, 1024, 256], P('row', 'col')
All inputs are finite; a program needn't handle non-finite values.
Results may differ from the reference program's by a relative error of at most 0.001.
Values are sent between devices in bfloat16 or wider.
A program may use at most 1 GiB of HBM per device.

```python
import jax
import jax.numpy as jnp
from jax import lax

GRID_ROWS = 4
GRID_COLS = 8
LAYERS = 2
NUM_STEPS = 3
BATCH_ROWS = 1024
D_MODEL = 256
D_FF = 1024

LEARN_RATE = 1.5
NORM_EPS = 1e-6
GELU_C = 0.7978845608028654
GELU_K = 0.044715
REPLICA_SPREAD = 0.5


def gelu_value(pre_act):
    tanh_inner = jnp.tanh(GELU_C * (pre_act + GELU_K * pre_act * pre_act * pre_act))
    return 0.5 * pre_act * (1.0 + tanh_inner)


def gelu_slope(pre_act):
    tanh_inner = jnp.tanh(GELU_C * (pre_act + GELU_K * pre_act * pre_act * pre_act))
    return 0.5 * (1.0 + tanh_inner) + 0.5 * pre_act * (1.0 - tanh_inner * tanh_inner) * GELU_C * (1.0 + 3.0 * GELU_K * pre_act * pre_act)


def setup_inputs(seed: int = 0) -> dict:
    root_key = jax.random.key(seed)
    sub_keys = jax.random.split(root_key, 6)
    grid_shape = (GRID_ROWS, GRID_COLS)
    shape_one = (LAYERS, D_MODEL, D_FF)
    shape_two = (LAYERS, D_FF, D_MODEL)
    norm_fac = (1.0 + REPLICA_SPREAD * REPLICA_SPREAD) ** -0.5
    base_one = jax.random.normal(sub_keys[0], shape_one, jnp.float32)
    own_one = jax.random.normal(sub_keys[1], grid_shape + shape_one, jnp.float32)
    w_one = (base_one + REPLICA_SPREAD * own_one) * (norm_fac * D_MODEL ** -0.5)
    base_two = jax.random.normal(sub_keys[2], shape_two, jnp.float32)
    own_two = jax.random.normal(sub_keys[3], grid_shape + shape_two, jnp.float32)
    w_two = (base_two + REPLICA_SPREAD * own_two) * (norm_fac * D_FF ** -0.5)
    data_shape = grid_shape + (NUM_STEPS, BATCH_ROWS, D_MODEL)
    inputs = jax.random.normal(sub_keys[4], data_shape, jnp.float32).astype(jnp.bfloat16)
    targets = jax.random.normal(sub_keys[5], data_shape, jnp.float32).astype(jnp.bfloat16)
    return {'w_one': w_one, 'w_two': w_two, 'inputs': inputs, 'targets': targets}


def local_update(w_one, w_two, x_in, target):
    one_lo = w_one.astype(jnp.bfloat16)
    two_lo = w_two.astype(jnp.bfloat16)
    hidden = x_in
    saved_acts = []
    for layer_idx in range(LAYERS):
        hid_f = hidden.astype(jnp.float32)
        inv_rms = lax.rsqrt(jnp.mean(hid_f * hid_f, axis=-1, keepdims=True) + NORM_EPS)
        normed = hid_f * inv_rms
        normed_lo = normed.astype(jnp.bfloat16)
        pre_act = jnp.dot(normed_lo, one_lo[layer_idx], preferred_element_type=jnp.float32)
        act_lo = gelu_value(pre_act).astype(jnp.bfloat16)
        mlp_out = jnp.dot(act_lo, two_lo[layer_idx], preferred_element_type=jnp.float32)
        saved_acts.append((normed, inv_rms, normed_lo, pre_act, act_lo))
        hidden = (hid_f + mlp_out).astype(jnp.bfloat16)
    d_hidden = (2.0 / (BATCH_ROWS * D_MODEL)) * (hidden.astype(jnp.float32) - target.astype(jnp.float32))
    grads_one = [None] * LAYERS
    grads_two = [None] * LAYERS
    for layer_idx in reversed(range(LAYERS)):
        normed, inv_rms, normed_lo, pre_act, act_lo = saved_acts[layer_idx]
        d_lo = d_hidden.astype(jnp.bfloat16)
        grads_two[layer_idx] = jnp.dot(act_lo.T, d_lo, preferred_element_type=jnp.float32)
        d_act = jnp.dot(d_lo, two_lo[layer_idx].T, preferred_element_type=jnp.float32)
        d_pre = (d_act * gelu_slope(pre_act)).astype(jnp.bfloat16)
        grads_one[layer_idx] = jnp.dot(normed_lo.T, d_pre, preferred_element_type=jnp.float32)
        if layer_idx > 0:
            d_normed = jnp.dot(d_pre, one_lo[layer_idx].T, preferred_element_type=jnp.float32)
            d_hidden = d_hidden + inv_rms * (d_normed - normed * jnp.mean(d_normed * normed, axis=-1, keepdims=True))
    return w_one - LEARN_RATE * jnp.stack(grads_one), w_two - LEARN_RATE * jnp.stack(grads_two)


def gossip_mix(upd_vals):
    wire_vals = upd_vals.astype(jnp.bfloat16)
    mix_sum = upd_vals + jnp.roll(wire_vals, 1, axis=1).astype(jnp.float32)
    mix_sum = mix_sum + jnp.roll(wire_vals, -1, axis=1).astype(jnp.float32)
    mix_sum = mix_sum + jnp.roll(wire_vals, 1, axis=0).astype(jnp.float32)
    mix_sum = mix_sum + jnp.roll(wire_vals, -1, axis=0).astype(jnp.float32)
    return mix_sum / 5.0


def reference(w_one, w_two, inputs, targets):
    n_rep = GRID_ROWS * GRID_COLS
    for step_idx in range(NUM_STEPS):
        flat_one = w_one.reshape((n_rep, LAYERS, D_MODEL, D_FF))
        flat_two = w_two.reshape((n_rep, LAYERS, D_FF, D_MODEL))
        x_step = inputs[:, :, step_idx].reshape((n_rep, BATCH_ROWS, D_MODEL))
        t_step = targets[:, :, step_idx].reshape((n_rep, BATCH_ROWS, D_MODEL))
        upd_one, upd_two = lax.map(lambda packed: local_update(packed[0], packed[1], packed[2], packed[3]), (flat_one, flat_two, x_step, t_step))
        w_one = gossip_mix(upd_one.reshape(w_one.shape))
        w_two = gossip_mix(upd_two.reshape(w_two.shape))
    return w_one, w_two
```

```python
import functools

import jax
import jax.numpy as jnp
from jax import lax
from jax.experimental import pallas as pl
from jax.experimental.pallas import tpu as pltpu
from jax.sharding import PartitionSpec as P

LEARN_RATE = 1.5
NORM_EPS = 1e-6
GELU_C = 0.7978845608028654
GELU_K = 0.044715

STEPS = 3
LAYERS = 2
BATCH = 1024
DM = 256
DF = 1024
FB = 256
NB = DF // FB
RT = 256
NR = BATCH // RT
MESH = pl.DeviceIdType.MESH
F32 = jnp.float32
BF16 = jnp.bfloat16

SEND_ORDER = [(1, 0), (0, 0), (0, 1), (0, 2), (0, 3), (1, 1), (1, 2), (1, 3)]


def dot_nn(a, b):
    return lax.dot_general(a, b, (((1,), (0,)), ((), ())), preferred_element_type=F32)


def dot_nt(a, b):
    return lax.dot_general(a, b, (((1,), (1,)), ((), ())), preferred_element_type=F32)


def dot_tn(a, b):
    return lax.dot_general(a, b, (((0,), (0,)), ((), ())), preferred_element_type=F32)


def kernel(n_rows, n_cols, w1_hbm, w2_hbm, a_hbm, t_hbm, o1_hbm, o2_hbm,
           wgt, wlo, wire, recv, ain, tin, nlo, nf1, inv1, act, slope, acc, err, elo, dzb, macc,
           load_sem, data_sem, send_sem, recv_sem, out_sem):
    row = lax.axis_index("row")
    col = lax.axis_index("col")
    targets = (
        (row, lax.rem(col + 1, n_cols)),
        (row, lax.rem(col + n_cols - 1, n_cols)),
        (lax.rem(row + 1, n_rows), col),
        (lax.rem(row + n_rows - 1, n_rows), col),
    )

    barrier = pltpu.get_barrier_semaphore()
    for tgt in targets:
        pl.semaphore_signal(barrier, inc=1, device_id=tgt, device_id_type=MESH)

    def load_one(layer, blk):
        return pltpu.make_async_copy(
            w1_hbm.at[layer, :, pl.ds(pl.multiple_of(blk * FB, FB), FB)], wgt.at[layer, blk, 0], load_sem.at[layer, blk, 0])

    def load_two(layer, blk):
        return pltpu.make_async_copy(
            w2_hbm.at[layer, pl.ds(pl.multiple_of(blk * FB, FB), FB), :], wgt.at[layer, blk, 1], load_sem.at[layer, blk, 1])

    def store_one(layer, blk):
        return pltpu.make_async_copy(
            wgt.at[layer, blk, 0], o1_hbm.at[layer, :, pl.ds(pl.multiple_of(blk * FB, FB), FB)], out_sem.at[layer, blk, 0])

    def store_two(layer, blk):
        return pltpu.make_async_copy(
            wgt.at[layer, blk, 1], o2_hbm.at[layer, pl.ds(pl.multiple_of(blk * FB, FB), FB), :], out_sem.at[layer, blk, 1])

    def load_a(step):
        return pltpu.make_async_copy(a_hbm.at[step], ain.at[step], data_sem.at[0, step])

    def load_t(step):
        return pltpu.make_async_copy(t_hbm.at[step], tin.at[step], data_sem.at[1, step])

    load_a(0).start()
    for layer in range(LAYERS):
        for blk in range(NB):
            load_one(layer, blk).start()
            load_two(layer, blk).start()
    load_t(0).start()
    for step in range(1, STEPS):
        load_a(step).start()
        load_t(step).start()

    def send(step, slot, layer, blk):
        par = lax.rem(step, 2)
        return pltpu.make_async_remote_copy(
            src_ref=wire.at[layer, blk],
            dst_ref=recv.at[par, slot, layer, blk],
            send_sem=send_sem.at[slot, layer, blk],
            recv_sem=recv_sem.at[par, slot, layer, blk],
            device_id=targets[slot],
            device_id_type=MESH,
        )

    def start_sends(step, layer, blk):
        for slot in (2, 3, 0, 1):
            send(step, slot, layer, blk).start()

    def combine(step, layer, blk, keep_lo):
        par = lax.rem(step, 2)
        for slot in range(4):
            send(step, slot, layer, blk).wait_recv()
        for which in range(2):
            @pl.loop(0, FB, step=64)
            def _(r0):
                rows = pl.ds(pl.multiple_of(r0, 64), 64)
                tot = wgt[layer, blk, which, rows]
                for slot in range(4):
                    tot = tot + recv[par, slot, layer, blk, which, rows].astype(F32)
                tot = tot * 0.2
                wgt[layer, blk, which, rows] = tot
                if keep_lo:
                    wlo[layer, blk, which, rows] = tot.astype(BF16)

    def normalise(step, layer):
        @pl.loop(0, BATCH, step=128)
        def _(r0):
            rows = pl.ds(pl.multiple_of(r0, 128), 128)
            if layer == 0:
                x = ain[step, rows].astype(F32)
            else:
                x = acc[rows].astype(BF16).astype(F32)
            inv = lax.rsqrt(jnp.mean(x * x, axis=-1, keepdims=True) + NORM_EPS)
            n = x * inv
            nlo[layer, rows] = n.astype(BF16)
            if layer == 1:
                nf1[rows] = n
                inv1[rows] = jnp.broadcast_to(inv, (128, 128))
            acc[rows] = x

    def forward_layer(step, layer):
        normalise(step, layer)

        @pl.loop(0, NB)
        def _(blk):
            @pl.when(step == 0)
            def _():
                load_one(layer, blk).wait()
                load_two(layer, blk).wait()
                for which in range(2):
                    @pl.loop(0, FB, step=64)
                    def _(r0):
                        rows = pl.ds(pl.multiple_of(r0, 64), 64)
                        wlo[layer, blk, which, rows] = wgt[layer, blk, which, rows].astype(BF16)

            @pl.when(step > 0)
            def _():
                combine(step - 1, layer, blk, True)

            w_one = wlo[layer, blk, 0]
            w_two = wlo[layer, blk, 1]
            for r in range(NR):
                rows = pl.ds(r * RT, RT)
                z = dot_nn(nlo[layer, rows], w_one)
                zz = z * z
                th = jnp.tanh(z * (GELU_C + (GELU_C * GELU_K) * zz))
                half = 0.5 + 0.5 * th
                slope[layer, blk, rows] = half + (0.5 * z) * (1.0 - th * th) * (GELU_C + (3.0 * GELU_C * GELU_K) * zz)
                a_lo = (z * half).astype(BF16)
                act[layer, blk, rows] = a_lo
                acc[rows] = acc[rows] + dot_nn(a_lo, w_two)

    def backward_layer(step, layer, send_now):
        if layer > 0:
            @pl.loop(0, BATCH, step=128)
            def _(r0):
                rows = pl.ds(pl.multiple_of(r0, 128), 128)
                macc[rows] = jnp.zeros((128, DM), F32)

        @pl.loop(0, NB)
        def _(blk):
            @pl.when(step > 0)
            def _():
                for slot in range(4):
                    send(step - 1, slot, layer, blk).wait_send()

            g_two = dot_tn(act[layer, blk], elo[...])
            q_two = wgt[layer, blk, 1] - LEARN_RATE * g_two
            wgt[layer, blk, 1] = q_two
            wire[layer, blk, 1] = q_two.astype(BF16)
            w_one = wlo[layer, blk, 0]
            w_two = wlo[layer, blk, 1]
            for r in range(NR):
                rows = pl.ds(r * RT, RT)
                u = dot_nt(elo[rows], w_two)
                dz = (u * slope[layer, blk, rows]).astype(BF16)
                dzb[rows] = dz
                if layer > 0:
                    macc[rows] = macc[rows] + dot_nt(dz, w_one)
            g_one = dot_tn(nlo[layer], dzb[...])
            q_one = wgt[layer, blk, 0] - LEARN_RATE * g_one
            wgt[layer, blk, 0] = q_one
            wire[layer, blk, 0] = q_one.astype(BF16)
            send_now(blk)

    @pl.loop(0, STEPS)
    def _(step):
        load_a(step).wait()
        forward_layer(step, 0)
        forward_layer(step, 1)

        load_t(step).wait()

        @pl.loop(0, BATCH, step=128)
        def _(r0):
            rows = pl.ds(pl.multiple_of(r0, 128), 128)
            e = (2.0 / (BATCH * DM)) * (acc[rows].astype(BF16).astype(F32) - tin[step, rows].astype(F32))
            err[rows] = e
            elo[rows] = e.astype(BF16)

        @pl.when(step == 0)
        def _():
            pl.semaphore_wait(barrier, 4)

        def send_first(blk):
            @pl.when(blk == 0)
            def _():
                start_sends(step, 1, 0)

        backward_layer(step, 1, send_first)

        @pl.loop(0, BATCH, step=128)
        def _(r0):
            rows = pl.ds(pl.multiple_of(r0, 128), 128)
            m = macc[rows]
            n = nf1[rows]
            inv = inv1[rows, 0:1]
            e = err[rows] + inv * (m - n * jnp.mean(m * n, axis=-1, keepdims=True))
            elo[rows] = e.astype(BF16)

        backward_layer(step, 0, lambda blk: start_sends(step, 0, blk))
        for blk in range(1, NB):
            start_sends(step, 1, blk)

    for layer, blk in SEND_ORDER:
        combine(STEPS - 1, layer, blk, False)
        store_one(layer, blk).start()
        store_two(layer, blk).start()
    for layer, blk in SEND_ORDER:
        for slot in range(4):
            send(STEPS - 1, slot, layer, blk).wait_send()
        store_one(layer, blk).wait()
        store_two(layer, blk).wait()


def solution(mesh):
    n_rows = mesh.shape["row"]
    n_cols = mesh.shape["col"]

    def device_fn(w_one, w_two, inputs, targets):
        chunk = (LAYERS, NB, 2, FB, DM)
        out_one, out_two = pl.pallas_call(
            functools.partial(kernel, n_rows, n_cols),
            out_shape=[
                jax.ShapeDtypeStruct((LAYERS, DM, DF), F32),
                jax.ShapeDtypeStruct((LAYERS, DF, DM), F32),
            ],
            in_specs=[pl.BlockSpec(memory_space=pl.ANY)] * 4,
            out_specs=[pl.BlockSpec(memory_space=pl.ANY)] * 2,
            scratch_shapes=[
                pltpu.VMEM(chunk, F32),
                pltpu.VMEM(chunk, BF16),
                pltpu.VMEM(chunk, BF16),
                pltpu.VMEM((2, 4) + chunk, BF16),
                pltpu.VMEM((STEPS, BATCH, DM), BF16),
                pltpu.VMEM((STEPS, BATCH, DM), BF16),
                pltpu.VMEM((LAYERS, BATCH, DM), BF16),
                pltpu.VMEM((BATCH, DM), F32),
                pltpu.VMEM((BATCH, 128), F32),
                pltpu.VMEM((LAYERS, NB, BATCH, FB), BF16),
                pltpu.VMEM((LAYERS, NB, BATCH, FB), F32),
                pltpu.VMEM((BATCH, DM), F32),
                pltpu.VMEM((BATCH, DM), F32),
                pltpu.VMEM((BATCH, DM), BF16),
                pltpu.VMEM((BATCH, FB), BF16),
                pltpu.VMEM((BATCH, DM), F32),
                pltpu.SemaphoreType.DMA((LAYERS, NB, 2)),
                pltpu.SemaphoreType.DMA((2, STEPS)),
                pltpu.SemaphoreType.DMA((4, LAYERS, NB)),
                pltpu.SemaphoreType.DMA((2, 4, LAYERS, NB)),
                pltpu.SemaphoreType.DMA((LAYERS, NB, 2)),
            ],
            compiler_params=pltpu.CompilerParams(
                collective_id=0, has_side_effects=True, vmem_limit_bytes=66 * 1000 * 1000),
        )(w_one[0, 0], w_two[0, 0], inputs[0, 0], targets[0, 0])
        return out_one[None, None], out_two[None, None]

    grid_spec = P("row", "col")
    return jax.shard_map(device_fn, mesh=mesh, in_specs=(grid_spec,) * 4, out_specs=(grid_spec,) * 2, check_vma=False)
```

```python
import functools

import jax
import jax.numpy as jnp
from jax import lax
from jax.experimental import pallas as pl
from jax.experimental.pallas import tpu as pltpu
from jax.sharding import PartitionSpec as P

LEARN_RATE = 1.5
NORM_EPS = 1e-6
GELU_C = 0.7978845608028654
GELU_K = 0.044715

STEPS = 3
LAYERS = 2
BATCH = 1024
DM = 256
DF = 1024
FB = 256
NB = DF // FB
RT = 256
NR = BATCH // RT
MESH = pl.DeviceIdType.MESH
F32 = jnp.float32
BF16 = jnp.bfloat16

SEND_ORDER = [(1, 0), (0, 0), (0, 1), (0, 2), (0, 3), (1, 1), (1, 2), (1, 3)]


def dot_nn(a, b):
    return lax.dot_general(a, b, (((1,), (0,)), ((), ())), preferred_element_type=F32)


def dot_nt(a, b):
    return lax.dot_general(a, b, (((1,), (1,)), ((), ())), preferred_element_type=F32)


def dot_tn(a, b):
    return lax.dot_general(a, b, (((0,), (0,)), ((), ())), preferred_element_type=F32)


def kernel(n_rows, n_cols, w1_hbm, w2_hbm, a_hbm, t_hbm, o1_hbm, o2_hbm,
           wgt, wlo, wire, recv, ain, tin, nlo, nf1, inv1, act, slope, acc, err, elo, dzb, macc,
           load_sem, data_sem, send_sem, recv_sem, relay_sem, out_sem):
    row = lax.axis_index("row")
    col = lax.axis_index("col")
    half = row // 2
    inner = jnp.logical_and(row > 0, row < n_rows - 1)
    targets = (
        ((row, lax.rem(col + 1, n_cols)), 0),
        ((row, lax.rem(col + n_cols - 1, n_cols)), 1),
        ((row + 1 - 2 * half, col), 2 + half),
        ((row - 1 + 2 * half, col), 3 - half),
    )
    relay_slot = 2 + half
    relay_target = ((3 - 3 * half, col), 3 - half)

    barrier = pltpu.get_barrier_semaphore()
    for shift in range(1, n_rows):
        pl.semaphore_signal(barrier, inc=1, device_id=(lax.rem(row + shift, n_rows), col), device_id_type=MESH)
    for tgt, _ in targets[:2]:
        pl.semaphore_signal(barrier, inc=1, device_id=tgt, device_id_type=MESH)

    def load_one(layer, blk):
        return pltpu.make_async_copy(
            w1_hbm.at[layer, :, pl.ds(pl.multiple_of(blk * FB, FB), FB)], wgt.at[layer, blk, 0], load_sem.at[layer, blk, 0])

    def load_two(layer, blk):
        return pltpu.make_async_copy(
            w2_hbm.at[layer, pl.ds(pl.multiple_of(blk * FB, FB), FB), :], wgt.at[layer, blk, 1], load_sem.at[layer, blk, 1])

    def store_one(layer, blk):
        return pltpu.make_async_copy(
            wgt.at[layer, blk, 0], o1_hbm.at[layer, :, pl.ds(pl.multiple_of(blk * FB, FB), FB)], out_sem.at[layer, blk, 0])

    def store_two(layer, blk):
        return pltpu.make_async_copy(
            wgt.at[layer, blk, 1], o2_hbm.at[layer, pl.ds(pl.multiple_of(blk * FB, FB), FB), :], out_sem.at[layer, blk, 1])

    def load_a(step):
        return pltpu.make_async_copy(a_hbm.at[step], ain.at[step], data_sem.at[0, step])

    def load_t(step):
        return pltpu.make_async_copy(t_hbm.at[step], tin.at[step], data_sem.at[1, step])

    load_a(0).start()
    for layer in range(LAYERS):
        for blk in range(NB):
            load_one(layer, blk).start()
            load_two(layer, blk).start()
    load_t(0).start()
    for step in range(1, STEPS):
        load_a(step).start()
        load_t(step).start()

    def send(step, kind, layer, blk):
        device, slot = targets[kind]
        return pltpu.make_async_remote_copy(
            src_ref=wire.at[layer, blk],
            dst_ref=recv.at[step, slot, layer, blk],
            send_sem=send_sem.at[kind, layer, blk],
            recv_sem=recv_sem.at[step, slot, layer, blk],
            device_id=device,
            device_id_type=MESH,
        )

    def relay(step, layer, blk):
        device, slot = relay_target
        return pltpu.make_async_remote_copy(
            src_ref=recv.at[step, relay_slot, layer, blk],
            dst_ref=recv.at[step, slot, layer, blk],
            send_sem=relay_sem.at[layer, blk],
            recv_sem=recv_sem.at[step, slot, layer, blk],
            device_id=device,
            device_id_type=MESH,
        )

    def arrival(step, slot, layer, blk):
        return pltpu.make_async_remote_copy(
            src_ref=wire.at[layer, blk],
            dst_ref=recv.at[step, slot, layer, blk],
            send_sem=send_sem.at[0, layer, blk],
            recv_sem=recv_sem.at[step, slot, layer, blk],
            device_id=targets[0][0],
            device_id_type=MESH,
        )

    def start_sends(step, layer, blk):
        for kind in (2, 0, 1):
            send(step, kind, layer, blk).start()

    def start_outward(step):
        @pl.when(inner)
        def _():
            @pl.when(step > 0)
            def _():
                for layer, blk in SEND_ORDER:
                    relay(step - 1, layer, blk).wait_send()
            for layer, blk in SEND_ORDER:
                send(step, 3, layer, blk).start()

    def wait_sends(step, layer, blk):
        for kind in range(3):
            send(step, kind, layer, blk).wait_send()

        @pl.when(inner)
        def _():
            send(step, 3, layer, blk).wait_send()

    def combine(step, layer, blk, keep_lo):
        arrival(step, relay_slot, layer, blk).wait_recv()

        @pl.when(inner)
        def _():
            relay(step, layer, blk).start()
        for slot in (0, 1, 5 - relay_slot):
            arrival(step, slot, layer, blk).wait_recv()
        for which in range(2):
            @pl.loop(0, FB, step=64)
            def _(r0):
                rows = pl.ds(pl.multiple_of(r0, 64), 64)
                tot = wgt[layer, blk, which, rows]
                for slot in range(4):
                    tot = tot + recv[step, slot, layer, blk, which, rows].astype(F32)
                tot = tot * 0.2
                wgt[layer, blk, which, rows] = tot
                if keep_lo:
                    wlo[layer, blk, which, rows] = tot.astype(BF16)

    def normalise(step, layer):
        @pl.loop(0, BATCH, step=128)
        def _(r0):
            rows = pl.ds(pl.multiple_of(r0, 128), 128)
            if layer == 0:
                x = ain[step, rows].astype(F32)
            else:
                x = acc[rows].astype(BF16).astype(F32)
            inv = lax.rsqrt(jnp.mean(x * x, axis=-1, keepdims=True) + NORM_EPS)
            n = x * inv
            nlo[layer, rows] = n.astype(BF16)
            if layer == 1:
                nf1[rows] = n
                inv1[rows] = jnp.broadcast_to(inv, (128, 128))
            acc[rows] = x

    def forward_layer(step, layer):
        normalise(step, layer)

        @pl.loop(0, NB)
        def _(blk):
            @pl.when(step == 0)
            def _():
                load_one(layer, blk).wait()
                load_two(layer, blk).wait()
                for which in range(2):
                    @pl.loop(0, FB, step=64)
                    def _(r0):
                        rows = pl.ds(pl.multiple_of(r0, 64), 64)
                        wlo[layer, blk, which, rows] = wgt[layer, blk, which, rows].astype(BF16)

            @pl.when(step > 0)
            def _():
                combine(step - 1, layer, blk, True)

            w_one = wlo[layer, blk, 0]
            w_two = wlo[layer, blk, 1]
            for r in range(NR):
                rows = pl.ds(r * RT, RT)
                z = dot_nn(nlo[layer, rows], w_one)
                zz = z * z
                th = jnp.tanh(z * (GELU_C + (GELU_C * GELU_K) * zz))
                half = 0.5 + 0.5 * th
                slope[layer, blk, rows] = half + (0.5 * z) * (1.0 - th * th) * (GELU_C + (3.0 * GELU_C * GELU_K) * zz)
                a_lo = (z * half).astype(BF16)
                act[layer, blk, rows] = a_lo
                acc[rows] = acc[rows] + dot_nn(a_lo, w_two)

    def backward_layer(step, layer, send_now):
        if layer > 0:
            @pl.loop(0, BATCH, step=128)
            def _(r0):
                rows = pl.ds(pl.multiple_of(r0, 128), 128)
                macc[rows] = jnp.zeros((128, DM), F32)

        @pl.loop(0, NB)
        def _(blk):
            @pl.when(step > 0)
            def _():
                wait_sends(step - 1, layer, blk)

            g_two = dot_tn(act[layer, blk], elo[...])
            q_two = wgt[layer, blk, 1] - LEARN_RATE * g_two
            wgt[layer, blk, 1] = q_two
            wire[layer, blk, 1] = q_two.astype(BF16)
            w_one = wlo[layer, blk, 0]
            w_two = wlo[layer, blk, 1]
            for r in range(NR):
                rows = pl.ds(r * RT, RT)
                u = dot_nt(elo[rows], w_two)
                dz = (u * slope[layer, blk, rows]).astype(BF16)
                dzb[rows] = dz
                if layer > 0:
                    macc[rows] = macc[rows] + dot_nt(dz, w_one)
            g_one = dot_tn(nlo[layer], dzb[...])
            q_one = wgt[layer, blk, 0] - LEARN_RATE * g_one
            wgt[layer, blk, 0] = q_one
            wire[layer, blk, 0] = q_one.astype(BF16)
            send_now(blk)

    pl.semaphore_wait(barrier, n_rows + 1)

    @pl.loop(0, STEPS)
    def _(step):
        load_a(step).wait()
        forward_layer(step, 0)
        forward_layer(step, 1)

        load_t(step).wait()

        @pl.loop(0, BATCH, step=128)
        def _(r0):
            rows = pl.ds(pl.multiple_of(r0, 128), 128)
            e = (2.0 / (BATCH * DM)) * (acc[rows].astype(BF16).astype(F32) - tin[step, rows].astype(F32))
            err[rows] = e
            elo[rows] = e.astype(BF16)

        def send_first(blk):
            @pl.when(blk == 0)
            def _():
                start_sends(step, 1, 0)

        backward_layer(step, 1, send_first)

        @pl.loop(0, BATCH, step=128)
        def _(r0):
            rows = pl.ds(pl.multiple_of(r0, 128), 128)
            m = macc[rows]
            n = nf1[rows]
            inv = inv1[rows, 0:1]
            e = err[rows] + inv * (m - n * jnp.mean(m * n, axis=-1, keepdims=True))
            elo[rows] = e.astype(BF16)

        backward_layer(step, 0, lambda blk: start_sends(step, 0, blk))
        for blk in range(1, NB):
            start_sends(step, 1, blk)
        start_outward(step)

    for layer, blk in SEND_ORDER:
        combine(STEPS - 1, layer, blk, False)
        store_one(layer, blk).start()
        store_two(layer, blk).start()
    for layer, blk in SEND_ORDER:
        wait_sends(STEPS - 1, layer, blk)

        @pl.when(inner)
        def _():
            relay(STEPS - 1, layer, blk).wait_send()
        store_one(layer, blk).wait()
        store_two(layer, blk).wait()


def solution(mesh):
    n_rows = mesh.shape["row"]
    n_cols = mesh.shape["col"]

    def device_fn(w_one, w_two, inputs, targets):
        chunk = (LAYERS, NB, 2, FB, DM)
        out_one, out_two = pl.pallas_call(
            functools.partial(kernel, n_rows, n_cols),
            out_shape=[
                jax.ShapeDtypeStruct((LAYERS, DM, DF), F32),
                jax.ShapeDtypeStruct((LAYERS, DF, DM), F32),
            ],
            in_specs=[pl.BlockSpec(memory_space=pl.ANY)] * 4,
            out_specs=[pl.BlockSpec(memory_space=pl.ANY)] * 2,
            scratch_shapes=[
                pltpu.VMEM(chunk, F32),
                pltpu.VMEM(chunk, BF16),
                pltpu.VMEM(chunk, BF16),
                pltpu.VMEM((STEPS, 4) + chunk, BF16),
                pltpu.VMEM((STEPS, BATCH, DM), BF16),
                pltpu.VMEM((STEPS, BATCH, DM), BF16),
                pltpu.VMEM((LAYERS, BATCH, DM), BF16),
                pltpu.VMEM((BATCH, DM), F32),
                pltpu.VMEM((BATCH, 128), F32),
                pltpu.VMEM((LAYERS, NB, BATCH, FB), BF16),
                pltpu.VMEM((LAYERS, NB, BATCH, FB), F32),
                pltpu.VMEM((BATCH, DM), F32),
                pltpu.VMEM((BATCH, DM), F32),
                pltpu.VMEM((BATCH, DM), BF16),
                pltpu.VMEM((BATCH, FB), BF16),
                pltpu.VMEM((BATCH, DM), F32),
                pltpu.SemaphoreType.DMA((LAYERS, NB, 2)),
                pltpu.SemaphoreType.DMA((2, STEPS)),
                pltpu.SemaphoreType.DMA((4, LAYERS, NB)),
                pltpu.SemaphoreType.DMA((STEPS, 4, LAYERS, NB)),
                pltpu.SemaphoreType.DMA((LAYERS, NB)),
                pltpu.SemaphoreType.DMA((LAYERS, NB, 2)),
            ],
            compiler_params=pltpu.CompilerParams(
                collective_id=0, has_side_effects=True, vmem_limit_bytes=66 * 1000 * 1000),
        )(w_one[0, 0], w_two[0, 0], inputs[0, 0], targets[0, 0])
        return out_one[None, None], out_two[None, None]

    grid_spec = P("row", "col")
    return jax.shard_map(device_fn, mesh=mesh, in_specs=(grid_spec,) * 4, out_specs=(grid_spec,) * 2, check_vma=False)
```

```python
import functools

import jax
import jax.numpy as jnp
from jax import lax
from jax.experimental import pallas as pl
from jax.experimental.pallas import tpu as pltpu
from jax.sharding import PartitionSpec as P

LEARN_RATE = 1.5
NORM_EPS = 1e-6
GELU_C = 0.7978845608028654
GELU_K = 0.044715

STEPS = 3
LAYERS = 2
BATCH = 1024
DM = 256
DF = 1024
FB = 256
NB = DF // FB
RT = 256
NR = BATCH // RT
MESH = pl.DeviceIdType.MESH
F32 = jnp.float32
BF16 = jnp.bfloat16

SEND_ORDER = [(1, 0), (0, 0), (0, 1), (0, 2), (0, 3), (1, 1), (1, 2), (1, 3)]


def dot_nn(a, b):
    return lax.dot_general(a, b, (((1,), (0,)), ((), ())), preferred_element_type=F32)


def dot_nt(a, b):
    return lax.dot_general(a, b, (((1,), (1,)), ((), ())), preferred_element_type=F32)


def dot_tn(a, b):
    return lax.dot_general(a, b, (((0,), (0,)), ((), ())), preferred_element_type=F32)


def kernel(n_rows, n_cols, w1_hbm, w2_hbm, a_hbm, t_hbm, o1_hbm, o2_hbm,
           wgt, wlo, wire, recv, ain, tin, nlo, nf1, inv1, act, slope, acc, err, elo, dzb, macc,
           load_sem, data_sem, send_sem, recv_sem, relay_sem, out_sem):
    row = lax.axis_index("row")
    col = lax.axis_index("col")
    half = row // 2
    inner = jnp.logical_and(row > 0, row < n_rows - 1)
    targets = (
        ((row, lax.rem(col + 1, n_cols)), 0),
        ((row, lax.rem(col + n_cols - 1, n_cols)), 1),
        ((row + 1 - 2 * half, col), 2 + half),
        ((row - 1 + 2 * half, col), 3 - half),
    )
    relay_slot = 2 + half
    relay_target = ((3 - 3 * half, col), 3 - half)

    barrier = pltpu.get_barrier_semaphore()
    for shift in range(1, n_rows):
        pl.semaphore_signal(barrier, inc=1, device_id=(lax.rem(row + shift, n_rows), col), device_id_type=MESH)
    for tgt, _ in targets[:2]:
        pl.semaphore_signal(barrier, inc=1, device_id=tgt, device_id_type=MESH)

    def load_one(layer, blk):
        return pltpu.make_async_copy(
            w1_hbm.at[layer, :, pl.ds(pl.multiple_of(blk * FB, FB), FB)], wgt.at[layer, blk, 0], load_sem.at[layer, blk, 0])

    def load_two(layer, blk):
        return pltpu.make_async_copy(
            w2_hbm.at[layer, pl.ds(pl.multiple_of(blk * FB, FB), FB), :], wgt.at[layer, blk, 1], load_sem.at[layer, blk, 1])

    def store_one(layer, blk):
        return pltpu.make_async_copy(
            wgt.at[layer, blk, 0], o1_hbm.at[layer, :, pl.ds(pl.multiple_of(blk * FB, FB), FB)], out_sem.at[layer, blk, 0])

    def store_two(layer, blk):
        return pltpu.make_async_copy(
            wgt.at[layer, blk, 1], o2_hbm.at[layer, pl.ds(pl.multiple_of(blk * FB, FB), FB), :], out_sem.at[layer, blk, 1])

    def load_a(step):
        return pltpu.make_async_copy(a_hbm.at[step], ain.at[step], data_sem.at[0, step])

    def load_t(step):
        return pltpu.make_async_copy(t_hbm.at[step], tin.at[step], data_sem.at[1, step])

    load_a(0).start()
    for layer in range(LAYERS):
        for blk in range(NB):
            load_one(layer, blk).start()
            load_two(layer, blk).start()
    load_t(0).start()
    for step in range(1, STEPS):
        load_a(step).start()
        load_t(step).start()

    def send(step, kind, layer, blk):
        device, slot = targets[kind]
        return pltpu.make_async_remote_copy(
            src_ref=wire.at[layer, blk],
            dst_ref=recv.at[step, slot, layer, blk],
            send_sem=send_sem.at[kind, layer, blk],
            recv_sem=recv_sem.at[step, slot, layer, blk],
            device_id=device,
            device_id_type=MESH,
        )

    def relay(step, layer, blk):
        device, slot = relay_target
        return pltpu.make_async_remote_copy(
            src_ref=recv.at[step, relay_slot, layer, blk],
            dst_ref=recv.at[step, slot, layer, blk],
            send_sem=relay_sem.at[layer, blk],
            recv_sem=recv_sem.at[step, slot, layer, blk],
            device_id=device,
            device_id_type=MESH,
        )

    def arrival(step, slot, layer, blk):
        return pltpu.make_async_remote_copy(
            src_ref=wire.at[layer, blk],
            dst_ref=recv.at[step, slot, layer, blk],
            send_sem=send_sem.at[0, layer, blk],
            recv_sem=recv_sem.at[step, slot, layer, blk],
            device_id=targets[0][0],
            device_id_type=MESH,
        )

    def start_sends(step, layer, blk):
        send(step, 2, layer, blk).start()

        @pl.when(jnp.logical_and(inner, step == 0))
        def _():
            send(step, 3, layer, blk).start()
        for kind in (0, 1):
            send(step, kind, layer, blk).start()

    def start_outward(step):
        @pl.when(jnp.logical_and(inner, step > 0))
        def _():
            for layer, blk in SEND_ORDER:
                relay(step - 1, layer, blk).wait_send()
            for layer, blk in SEND_ORDER:
                send(step, 3, layer, blk).start()

    def wait_sends(step, layer, blk):
        for kind in range(3):
            send(step, kind, layer, blk).wait_send()

        @pl.when(inner)
        def _():
            send(step, 3, layer, blk).wait_send()

    def combine(step, layer, blk, keep_lo):
        arrival(step, relay_slot, layer, blk).wait_recv()

        @pl.when(inner)
        def _():
            relay(step, layer, blk).start()
        for slot in (0, 1, 5 - relay_slot):
            arrival(step, slot, layer, blk).wait_recv()
        for which in range(2):
            @pl.loop(0, FB, step=64)
            def _(r0):
                rows = pl.ds(pl.multiple_of(r0, 64), 64)
                tot = wgt[layer, blk, which, rows]
                for slot in range(4):
                    tot = tot + recv[step, slot, layer, blk, which, rows].astype(F32)
                tot = tot * 0.2
                wgt[layer, blk, which, rows] = tot
                if keep_lo:
                    wlo[layer, blk, which, rows] = tot.astype(BF16)

    def normalise(step, layer):
        @pl.loop(0, BATCH, step=128)
        def _(r0):
            rows = pl.ds(pl.multiple_of(r0, 128), 128)
            if layer == 0:
                x = ain[step, rows].astype(F32)
            else:
                x = acc[rows].astype(BF16).astype(F32)
            inv = lax.rsqrt(jnp.mean(x * x, axis=-1, keepdims=True) + NORM_EPS)
            n = x * inv
            nlo[layer, rows] = n.astype(BF16)
            if layer == 1:
                nf1[rows] = n
                inv1[rows] = jnp.broadcast_to(inv, (128, 128))
            acc[rows] = x

    def forward_layer(step, layer, first):
        normalise(step, layer)

        @pl.loop(0, NB)
        def _(blk):
            if first:
                load_one(layer, blk).wait()
                load_two(layer, blk).wait()
                for which in range(2):
                    @pl.loop(0, FB, step=64)
                    def _(r0):
                        rows = pl.ds(pl.multiple_of(r0, 64), 64)
                        wlo[layer, blk, which, rows] = wgt[layer, blk, which, rows].astype(BF16)
            else:
                combine(step - 1, layer, blk, True)

            w_one = wlo[layer, blk, 0]
            w_two = wlo[layer, blk, 1]
            for r in range(NR):
                rows = pl.ds(r * RT, RT)
                z = dot_nn(nlo[layer, rows], w_one)
                zz = z * z
                th = jnp.tanh(z * (GELU_C + (GELU_C * GELU_K) * zz))
                half = 0.5 + 0.5 * th
                slope[layer, blk, rows] = half + (0.5 * z) * (1.0 - th * th) * (GELU_C + (3.0 * GELU_C * GELU_K) * zz)
                a_lo = (z * half).astype(BF16)
                act[layer, blk, rows] = a_lo
                acc[rows] = acc[rows] + dot_nn(a_lo, w_two)

    def backward_layer(step, layer, send_now):
        if layer > 0:
            @pl.loop(0, BATCH, step=128)
            def _(r0):
                rows = pl.ds(pl.multiple_of(r0, 128), 128)
                macc[rows] = jnp.zeros((128, DM), F32)

        @pl.loop(0, NB)
        def _(blk):
            @pl.when(step > 0)
            def _():
                wait_sends(step - 1, layer, blk)

            g_two = dot_tn(act[layer, blk], elo[...])
            q_two = wgt[layer, blk, 1] - LEARN_RATE * g_two
            wgt[layer, blk, 1] = q_two
            wire[layer, blk, 1] = q_two.astype(BF16)
            w_one = wlo[layer, blk, 0]
            w_two = wlo[layer, blk, 1]
            for r in range(NR):
                rows = pl.ds(r * RT, RT)
                u = dot_nt(elo[rows], w_two)
                dz = (u * slope[layer, blk, rows]).astype(BF16)
                dzb[rows] = dz
                if layer > 0:
                    macc[rows] = macc[rows] + dot_nt(dz, w_one)
            g_one = dot_tn(nlo[layer], dzb[...])
            q_one = wgt[layer, blk, 0] - LEARN_RATE * g_one
            wgt[layer, blk, 0] = q_one
            wire[layer, blk, 0] = q_one.astype(BF16)
            send_now(blk)

    def forward(step, first):
        load_a(step).wait()
        with jax.named_scope("fwd0"):
            forward_layer(step, 0, first)
        with jax.named_scope("fwd1"):
            forward_layer(step, 1, first)

    forward(0, True)
    pl.semaphore_wait(barrier, n_rows + 1)

    @pl.loop(0, STEPS)
    def _(step):
        load_t(step).wait()

        @pl.loop(0, BATCH, step=128)
        def _(r0):
            rows = pl.ds(pl.multiple_of(r0, 128), 128)
            e = (2.0 / (BATCH * DM)) * (acc[rows].astype(BF16).astype(F32) - tin[step, rows].astype(F32))
            err[rows] = e
            elo[rows] = e.astype(BF16)

        def send_first(blk):
            @pl.when(blk == 0)
            def _():
                start_sends(step, 1, 0)

        backward_layer(step, 1, send_first)

        @pl.loop(0, BATCH, step=128)
        def _(r0):
            rows = pl.ds(pl.multiple_of(r0, 128), 128)
            m = macc[rows]
            n = nf1[rows]
            inv = inv1[rows, 0:1]
            e = err[rows] + inv * (m - n * jnp.mean(m * n, axis=-1, keepdims=True))
            elo[rows] = e.astype(BF16)

        backward_layer(step, 0, lambda blk: start_sends(step, 0, blk))
        for blk in range(1, NB):
            start_sends(step, 1, blk)
        start_outward(step)

        @pl.when(step < STEPS - 1)
        def _():
            forward(step + 1, False)

    for layer, blk in SEND_ORDER:
        combine(STEPS - 1, layer, blk, False)
        store_one(layer, blk).start()
        store_two(layer, blk).start()
    for layer, blk in SEND_ORDER:
        wait_sends(STEPS - 1, layer, blk)

        @pl.when(inner)
        def _():
            relay(STEPS - 1, layer, blk).wait_send()
        store_one(layer, blk).wait()
        store_two(layer, blk).wait()


def solution(mesh):
    n_rows = mesh.shape["row"]
    n_cols = mesh.shape["col"]

    def device_fn(w_one, w_two, inputs, targets):
        chunk = (LAYERS, NB, 2, FB, DM)
        out_one, out_two = pl.pallas_call(
            functools.partial(kernel, n_rows, n_cols),
            out_shape=[
                jax.ShapeDtypeStruct((LAYERS, DM, DF), F32),
                jax.ShapeDtypeStruct((LAYERS, DF, DM), F32),
            ],
            in_specs=[pl.BlockSpec(memory_space=pl.ANY)] * 4,
            out_specs=[pl.BlockSpec(memory_space=pl.ANY)] * 2,
            scratch_shapes=[
                pltpu.VMEM(chunk, F32),
                pltpu.VMEM(chunk, BF16),
                pltpu.VMEM(chunk, BF16),
                pltpu.VMEM((STEPS, 4) + chunk, BF16),
                pltpu.VMEM((STEPS, BATCH, DM), BF16),
                pltpu.VMEM((STEPS, BATCH, DM), BF16),
                pltpu.VMEM((LAYERS, BATCH, DM), BF16),
                pltpu.VMEM((BATCH, DM), F32),
                pltpu.VMEM((BATCH, 128), F32),
                pltpu.VMEM((LAYERS, NB, BATCH, FB), BF16),
                pltpu.VMEM((LAYERS, NB, BATCH, FB), F32),
                pltpu.VMEM((BATCH, DM), F32),
                pltpu.VMEM((BATCH, DM), F32),
                pltpu.VMEM((BATCH, DM), BF16),
                pltpu.VMEM((BATCH, FB), BF16),
                pltpu.VMEM((BATCH, DM), F32),
                pltpu.SemaphoreType.DMA((LAYERS, NB, 2)),
                pltpu.SemaphoreType.DMA((2, STEPS)),
                pltpu.SemaphoreType.DMA((4, LAYERS, NB)),
                pltpu.SemaphoreType.DMA((STEPS, 4, LAYERS, NB)),
                pltpu.SemaphoreType.DMA((LAYERS, NB)),
                pltpu.SemaphoreType.DMA((LAYERS, NB, 2)),
            ],
            compiler_params=pltpu.CompilerParams(
                collective_id=0, has_side_effects=True, vmem_limit_bytes=66 * 1000 * 1000),
        )(w_one[0, 0], w_two[0, 0], inputs[0, 0], targets[0, 0])
        return out_one[None, None], out_two[None, None]

    grid_spec = P("row", "col")
    return jax.shard_map(device_fn, mesh=mesh, in_specs=(grid_spec,) * 4, out_specs=(grid_spec,) * 2, check_vma=False)
```

```python
import functools

import jax
import jax.numpy as jnp
from jax import lax
from jax.experimental import pallas as pl
from jax.experimental.pallas import tpu as pltpu
from jax.sharding import PartitionSpec as P

LEARN_RATE = 1.5
NORM_EPS = 1e-6
GELU_C = 0.7978845608028654
GELU_K = 0.044715

STEPS = 3
LAYERS = 2
BATCH = 1024
DM = 256
DF = 1024
FB = 256
NB = DF // FB
RT = 256
NR = BATCH // RT
MESH = pl.DeviceIdType.MESH
F32 = jnp.float32
BF16 = jnp.bfloat16

SEND_ORDER = [(1, 0), (0, 0), (0, 1), (0, 2), (0, 3), (1, 1), (1, 2), (1, 3)]


def dot_nn(a, b):
    return lax.dot_general(a, b, (((1,), (0,)), ((), ())), preferred_element_type=F32)


def dot_nt(a, b):
    return lax.dot_general(a, b, (((1,), (1,)), ((), ())), preferred_element_type=F32)


def dot_tn(a, b):
    return lax.dot_general(a, b, (((0,), (0,)), ((), ())), preferred_element_type=F32)


def kernel(n_rows, n_cols, w1_hbm, w2_hbm, a_hbm, t_hbm, wgt,
           wlo, wire, recv, ain, tin, nlo, nf1, inv1, act, slope, acc, err, elo, dzb, macc,
           load_sem, data_sem, send_sem, recv_sem, relay_sem):
    row = lax.axis_index("row")
    col = lax.axis_index("col")
    half = row // 2
    inner = jnp.logical_and(row > 0, row < n_rows - 1)
    targets = (
        ((row, lax.rem(col + 1, n_cols)), 0),
        ((row, lax.rem(col + n_cols - 1, n_cols)), 1),
        ((row + 1 - 2 * half, col), 2 + half),
        ((row - 1 + 2 * half, col), 3 - half),
    )
    relay_slot = 2 + half
    relay_target = ((3 - 3 * half, col), 3 - half)

    barrier = pltpu.get_barrier_semaphore()
    for shift in range(1, n_rows):
        pl.semaphore_signal(barrier, inc=1, device_id=(lax.rem(row + shift, n_rows), col), device_id_type=MESH)
    for tgt, _ in targets[:2]:
        pl.semaphore_signal(barrier, inc=1, device_id=tgt, device_id_type=MESH)

    def load_one(layer, blk):
        return pltpu.make_async_copy(
            w1_hbm.at[layer, :, pl.ds(pl.multiple_of(blk * FB, FB), FB)], wgt.at[layer, blk, 0], load_sem.at[layer, blk, 0])

    def load_two(layer, blk):
        return pltpu.make_async_copy(
            w2_hbm.at[layer, pl.ds(pl.multiple_of(blk * FB, FB), FB), :], wgt.at[layer, blk, 1], load_sem.at[layer, blk, 1])

    def load_a(step):
        return pltpu.make_async_copy(a_hbm.at[step], ain.at[step], data_sem.at[0, step])

    def load_t(step):
        return pltpu.make_async_copy(t_hbm.at[step], tin.at[step], data_sem.at[1, step])

    load_a(0).start()
    for layer in range(LAYERS):
        for blk in range(NB):
            load_one(layer, blk).start()
            load_two(layer, blk).start()
    load_t(0).start()
    for step in range(1, STEPS):
        load_a(step).start()
        load_t(step).start()

    def send(step, kind, layer, blk):
        device, slot = targets[kind]
        return pltpu.make_async_remote_copy(
            src_ref=wire.at[layer, blk],
            dst_ref=recv.at[step, slot, layer, blk],
            send_sem=send_sem.at[kind, layer, blk],
            recv_sem=recv_sem.at[step, slot, layer, blk],
            device_id=device,
            device_id_type=MESH,
        )

    def relay(step, layer, blk):
        device, slot = relay_target
        return pltpu.make_async_remote_copy(
            src_ref=recv.at[step, relay_slot, layer, blk],
            dst_ref=recv.at[step, slot, layer, blk],
            send_sem=relay_sem.at[layer, blk],
            recv_sem=recv_sem.at[step, slot, layer, blk],
            device_id=device,
            device_id_type=MESH,
        )

    def arrival(step, slot, layer, blk):
        return pltpu.make_async_remote_copy(
            src_ref=wire.at[layer, blk],
            dst_ref=recv.at[step, slot, layer, blk],
            send_sem=send_sem.at[0, layer, blk],
            recv_sem=recv_sem.at[step, slot, layer, blk],
            device_id=targets[0][0],
            device_id_type=MESH,
        )

    def start_sends(step, layer, blk):
        send(step, 2, layer, blk).start()

        @pl.when(jnp.logical_and(inner, step == 0))
        def _():
            send(step, 3, layer, blk).start()
        for kind in (0, 1):
            send(step, kind, layer, blk).start()

    def start_outward(step):
        @pl.when(jnp.logical_and(inner, step > 0))
        def _():
            for layer, blk in SEND_ORDER:
                relay(step - 1, layer, blk).wait_send()
            for layer, blk in SEND_ORDER:
                send(step, 3, layer, blk).start()

    def wait_sends(step, layer, blk):
        for kind in range(3):
            send(step, kind, layer, blk).wait_send()

        @pl.when(inner)
        def _():
            send(step, 3, layer, blk).wait_send()

    def combine(step, layer, blk, keep_lo):
        arrival(step, relay_slot, layer, blk).wait_recv()

        @pl.when(inner)
        def _():
            relay(step, layer, blk).start()
        for slot in (0, 1, 5 - relay_slot):
            arrival(step, slot, layer, blk).wait_recv()
        for which in range(2):
            @pl.loop(0, FB, step=64)
            def _(r0):
                rows = pl.ds(pl.multiple_of(r0, 64), 64)
                tot = wgt[layer, blk, which, rows]
                for slot in range(4):
                    tot = tot + recv[step, slot, layer, blk, which, rows].astype(F32)
                tot = tot * 0.2
                wgt[layer, blk, which, rows] = tot
                if keep_lo:
                    wlo[layer, blk, which, rows] = tot.astype(BF16)

    def normalise(step, layer):
        @pl.loop(0, BATCH, step=128)
        def _(r0):
            rows = pl.ds(pl.multiple_of(r0, 128), 128)
            if layer == 0:
                x = ain[step, rows].astype(F32)
            else:
                x = acc[rows].astype(BF16).astype(F32)
            inv = lax.rsqrt(jnp.mean(x * x, axis=-1, keepdims=True) + NORM_EPS)
            n = x * inv
            nlo[layer, rows] = n.astype(BF16)
            if layer == 1:
                nf1[rows] = n
                inv1[rows] = jnp.broadcast_to(inv, (128, 128))
            acc[rows] = x

    def forward_layer(step, layer, first):
        normalise(step, layer)

        @pl.loop(0, NB)
        def _(blk):
            if first:
                load_one(layer, blk).wait()
                load_two(layer, blk).wait()
                for which in range(2):
                    @pl.loop(0, FB, step=64)
                    def _(r0):
                        rows = pl.ds(pl.multiple_of(r0, 64), 64)
                        wlo[layer, blk, which, rows] = wgt[layer, blk, which, rows].astype(BF16)
            else:
                combine(step - 1, layer, blk, True)

            w_one = wlo[layer, blk, 0]
            w_two = wlo[layer, blk, 1]
            for r in range(NR):
                rows = pl.ds(r * RT, RT)
                z = dot_nn(nlo[layer, rows], w_one)
                zz = z * z
                th = jnp.tanh(z * (GELU_C + (GELU_C * GELU_K) * zz))
                half = 0.5 + 0.5 * th
                slope[layer, blk, rows] = half + (0.5 * z) * (1.0 - th * th) * (GELU_C + (3.0 * GELU_C * GELU_K) * zz)
                a_lo = (z * half).astype(BF16)
                act[layer, blk, rows] = a_lo
                acc[rows] = acc[rows] + dot_nn(a_lo, w_two)

    def backward_layer(step, layer, send_now):
        if layer > 0:
            @pl.loop(0, BATCH, step=128)
            def _(r0):
                rows = pl.ds(pl.multiple_of(r0, 128), 128)
                macc[rows] = jnp.zeros((128, DM), F32)

        @pl.loop(0, NB)
        def _(blk):
            @pl.when(step > 0)
            def _():
                wait_sends(step - 1, layer, blk)

            g_two = dot_tn(act[layer, blk], elo[...])
            q_two = wgt[layer, blk, 1] - LEARN_RATE * g_two
            wgt[layer, blk, 1] = q_two
            wire[layer, blk, 1] = q_two.astype(BF16)
            w_one = wlo[layer, blk, 0]
            w_two = wlo[layer, blk, 1]
            for r in range(NR):
                rows = pl.ds(r * RT, RT)
                u = dot_nt(elo[rows], w_two)
                dz = (u * slope[layer, blk, rows]).astype(BF16)
                dzb[rows] = dz
                if layer > 0:
                    macc[rows] = macc[rows] + dot_nt(dz, w_one)
            g_one = dot_tn(nlo[layer], dzb[...])
            q_one = wgt[layer, blk, 0] - LEARN_RATE * g_one
            wgt[layer, blk, 0] = q_one
            wire[layer, blk, 0] = q_one.astype(BF16)
            send_now(blk)

    def forward(step, first):
        load_a(step).wait()
        with jax.named_scope("fwd0"):
            forward_layer(step, 0, first)
        with jax.named_scope("fwd1"):
            forward_layer(step, 1, first)

    forward(0, True)
    pl.semaphore_wait(barrier, n_rows + 1)

    @pl.loop(0, STEPS)
    def _(step):
        load_t(step).wait()

        @pl.loop(0, BATCH, step=128)
        def _(r0):
            rows = pl.ds(pl.multiple_of(r0, 128), 128)
            e = (2.0 / (BATCH * DM)) * (acc[rows].astype(BF16).astype(F32) - tin[step, rows].astype(F32))
            err[rows] = e
            elo[rows] = e.astype(BF16)

        def send_first(blk):
            @pl.when(blk == 0)
            def _():
                start_sends(step, 1, 0)

        backward_layer(step, 1, send_first)

        @pl.loop(0, BATCH, step=128)
        def _(r0):
            rows = pl.ds(pl.multiple_of(r0, 128), 128)
            m = macc[rows]
            n = nf1[rows]
            inv = inv1[rows, 0:1]
            e = err[rows] + inv * (m - n * jnp.mean(m * n, axis=-1, keepdims=True))
            elo[rows] = e.astype(BF16)

        backward_layer(step, 0, lambda blk: start_sends(step, 0, blk))
        for blk in range(1, NB):
            start_sends(step, 1, blk)
        start_outward(step)

        @pl.when(step < STEPS - 1)
        def _():
            forward(step + 1, False)

    for layer, blk in SEND_ORDER:
        combine(STEPS - 1, layer, blk, False)
    for layer, blk in SEND_ORDER:
        wait_sends(STEPS - 1, layer, blk)

        @pl.when(inner)
        def _():
            relay(STEPS - 1, layer, blk).wait_send()


def store_kernel(wgt, o1_hbm, o2_hbm, out_sem):
    copies = []
    for layer in range(LAYERS):
        for blk in range(NB):
            span = pl.ds(blk * FB, FB)
            copies.append(pltpu.make_async_copy(wgt.at[layer, blk, 0], o1_hbm.at[layer, :, span], out_sem.at[layer, blk, 0]))
            copies.append(pltpu.make_async_copy(wgt.at[layer, blk, 1], o2_hbm.at[layer, span, :], out_sem.at[layer, blk, 1]))
    for copy in copies:
        copy.start()
    for copy in copies:
        copy.wait()


def solution(mesh):
    n_rows = mesh.shape["row"]
    n_cols = mesh.shape["col"]

    def device_fn(w_one, w_two, inputs, targets):
        chunk = (LAYERS, NB, 2, FB, DM)
        weights = pl.pallas_call(
            functools.partial(kernel, n_rows, n_cols),
            out_shape=pltpu.VMEM(chunk, F32),
            in_specs=[pl.BlockSpec(memory_space=pl.ANY)] * 4,
            out_specs=pl.BlockSpec(memory_space=pltpu.VMEM),
            scratch_shapes=[
                pltpu.VMEM(chunk, BF16),
                pltpu.VMEM(chunk, BF16),
                pltpu.VMEM((STEPS, 4) + chunk, BF16),
                pltpu.VMEM((STEPS, BATCH, DM), BF16),
                pltpu.VMEM((STEPS, BATCH, DM), BF16),
                pltpu.VMEM((LAYERS, BATCH, DM), BF16),
                pltpu.VMEM((BATCH, DM), F32),
                pltpu.VMEM((BATCH, 128), F32),
                pltpu.VMEM((LAYERS, NB, BATCH, FB), BF16),
                pltpu.VMEM((LAYERS, NB, BATCH, FB), F32),
                pltpu.VMEM((BATCH, DM), F32),
                pltpu.VMEM((BATCH, DM), F32),
                pltpu.VMEM((BATCH, DM), BF16),
                pltpu.VMEM((BATCH, FB), BF16),
                pltpu.VMEM((BATCH, DM), F32),
                pltpu.SemaphoreType.DMA((LAYERS, NB, 2)),
                pltpu.SemaphoreType.DMA((2, STEPS)),
                pltpu.SemaphoreType.DMA((4, LAYERS, NB)),
                pltpu.SemaphoreType.DMA((STEPS, 4, LAYERS, NB)),
                pltpu.SemaphoreType.DMA((LAYERS, NB)),
            ],
            compiler_params=pltpu.CompilerParams(
                collective_id=0, has_side_effects=True, vmem_limit_bytes=58 * 2**20),
        )(w_one[0, 0], w_two[0, 0], inputs[0, 0], targets[0, 0])
        out_one, out_two = pl.pallas_call(
            store_kernel,
            out_shape=[
                jax.ShapeDtypeStruct((LAYERS, DM, DF), F32),
                jax.ShapeDtypeStruct((LAYERS, DF, DM), F32),
            ],
            in_specs=[pl.BlockSpec(memory_space=pltpu.VMEM)],
            out_specs=[pl.BlockSpec(memory_space=pl.ANY)] * 2,
            scratch_shapes=[pltpu.SemaphoreType.DMA((LAYERS, NB, 2))],
            compiler_params=pltpu.CompilerParams(vmem_limit_bytes=2**20),
        )(weights)
        return out_one[None, None], out_two[None, None]

    grid_spec = P("row", "col")
    return jax.shard_map(device_fn, mesh=mesh, in_specs=(grid_spec,) * 4, out_specs=(grid_spec,) * 2, check_vma=False)
```

```python
import functools

import jax
import jax.numpy as jnp
from jax import lax
from jax.experimental import pallas as pl
from jax.experimental.pallas import tpu as pltpu
from jax.sharding import PartitionSpec as P

LEARN_RATE = 1.5
NORM_EPS = 1e-6
GELU_C = 0.7978845608028654
GELU_K = 0.044715

STEPS = 3
LAYERS = 2
BATCH = 1024
DM = 256
DF = 1024
FB = 256
NB = DF // FB
RT = 256
NR = BATCH // RT
MESH = pl.DeviceIdType.MESH
F32 = jnp.float32
BF16 = jnp.bfloat16

EARLY = 2
SEND_ORDER = [(1, b) for b in range(EARLY)] + [(0, b) for b in range(NB)] + [(1, b) for b in range(EARLY, NB)]


def dot_nn(a, b):
    return lax.dot_general(a, b, (((1,), (0,)), ((), ())), preferred_element_type=F32)


def dot_nt(a, b):
    return lax.dot_general(a, b, (((1,), (1,)), ((), ())), preferred_element_type=F32)


def dot_tn(a, b):
    return lax.dot_general(a, b, (((0,), (0,)), ((), ())), preferred_element_type=F32)


def kernel(n_rows, n_cols, w1_hbm, w2_hbm, a_hbm, t_hbm, wgt,
           wlo, wire, recv, ain, tin, nlo, nf1, inv1, act, pre, acc, err, elo, dzb, macc,
           load_sem, data_sem, send_sem, recv_sem, relay_sem):
    row = lax.axis_index("row")
    col = lax.axis_index("col")
    half = row // 2
    inner = jnp.logical_and(row > 0, row < n_rows - 1)
    targets = (
        ((row, lax.rem(col + 1, n_cols)), 0),
        ((row, lax.rem(col + n_cols - 1, n_cols)), 1),
        ((row + 1 - 2 * half, col), 2 + half),
        ((row - 1 + 2 * half, col), 3 - half),
    )
    relay_slot = 2 + half
    relay_target = ((3 - 3 * half, col), 3 - half)

    def load_one(layer, blk):
        return pltpu.make_async_copy(
            w1_hbm.at[layer, :, pl.ds(pl.multiple_of(blk * FB, FB), FB)], wgt.at[layer, blk, 0], load_sem.at[layer, blk, 0])

    def load_two(layer, blk):
        return pltpu.make_async_copy(
            w2_hbm.at[layer, pl.ds(pl.multiple_of(blk * FB, FB), FB), :], wgt.at[layer, blk, 1], load_sem.at[layer, blk, 1])

    def load_a(step):
        return pltpu.make_async_copy(a_hbm.at[step], ain.at[step], data_sem.at[0, step])

    def load_t(step):
        return pltpu.make_async_copy(t_hbm.at[step], tin.at[step], data_sem.at[1, step])

    load_a(0).start()
    for blk in range(NB):
        load_one(0, blk).start()
        load_two(0, blk).start()

    barrier = pltpu.get_barrier_semaphore()
    for shift in range(1, n_rows):
        pl.semaphore_signal(barrier, inc=1, device_id=(lax.rem(row + shift, n_rows), col), device_id_type=MESH)
    for tgt, _ in targets[:2]:
        pl.semaphore_signal(barrier, inc=1, device_id=tgt, device_id_type=MESH)

    for blk in range(NB):
        load_one(1, blk).start()
        load_two(1, blk).start()
    load_t(0).start()
    for step in range(1, STEPS):
        load_a(step).start()
        load_t(step).start()

    def send(step, kind, layer, blk):
        device, slot = targets[kind]
        return pltpu.make_async_remote_copy(
            src_ref=wire.at[layer, blk],
            dst_ref=recv.at[step, slot, layer, blk],
            send_sem=send_sem.at[kind, layer, blk],
            recv_sem=recv_sem.at[step, slot, layer, blk],
            device_id=device,
            device_id_type=MESH,
        )

    def relay(step, layer, blk):
        device, slot = relay_target
        return pltpu.make_async_remote_copy(
            src_ref=recv.at[step, relay_slot, layer, blk],
            dst_ref=recv.at[step, slot, layer, blk],
            send_sem=relay_sem.at[layer, blk],
            recv_sem=recv_sem.at[step, slot, layer, blk],
            device_id=device,
            device_id_type=MESH,
        )

    def arrival(step, slot, layer, blk):
        return pltpu.make_async_remote_copy(
            src_ref=wire.at[layer, blk],
            dst_ref=recv.at[step, slot, layer, blk],
            send_sem=send_sem.at[0, layer, blk],
            recv_sem=recv_sem.at[step, slot, layer, blk],
            device_id=targets[0][0],
            device_id_type=MESH,
        )

    def start_sends(step, layer, blk):
        send(step, 2, layer, blk).start()

        @pl.when(jnp.logical_and(inner, step == 0))
        def _():
            send(step, 3, layer, blk).start()
        for kind in (0, 1):
            send(step, kind, layer, blk).start()

    def start_outward(step):
        @pl.when(jnp.logical_and(inner, step > 0))
        def _():
            for layer, blk in SEND_ORDER:
                relay(step - 1, layer, blk).wait_send()
            for layer, blk in SEND_ORDER:
                send(step, 3, layer, blk).start()

    def wait_sends(step, layer, blk):
        for kind in range(3):
            send(step, kind, layer, blk).wait_send()

        @pl.when(inner)
        def _():
            send(step, 3, layer, blk).wait_send()

    def combine(step, layer, blk, keep_lo):
        arrival(step, relay_slot, layer, blk).wait_recv()

        @pl.when(inner)
        def _():
            relay(step, layer, blk).start()
        for slot in (0, 1, 5 - relay_slot):
            arrival(step, slot, layer, blk).wait_recv()
        for which in range(2):
            @pl.loop(0, FB, step=64)
            def _(r0):
                rows = pl.ds(pl.multiple_of(r0, 64), 64)
                tot = wgt[layer, blk, which, rows]
                for slot in range(4):
                    tot = tot + recv[step, slot, layer, blk, which, rows].astype(F32)
                tot = tot * 0.2
                wgt[layer, blk, which, rows] = tot
                if keep_lo:
                    wlo[layer, blk, which, rows] = tot.astype(BF16)

    def normalise(step, layer):
        for r0 in range(0, BATCH, 128):
            rows = pl.ds(r0, 128)
            if layer == 0:
                x = ain[step, rows].astype(F32)
            else:
                x = acc[rows].astype(BF16).astype(F32)
            inv = lax.rsqrt(jnp.mean(x * x, axis=-1, keepdims=True) + NORM_EPS)
            n = x * inv
            nlo[layer, rows] = n.astype(BF16)
            if layer == 1:
                nf1[rows] = n
                inv1[rows] = jnp.broadcast_to(inv, (128, 128))
            acc[rows] = x

    def forward_layer(step, layer, first):
        normalise(step, layer)

        @pl.loop(0, NB)
        def _(blk):
            if first:
                load_one(layer, blk).wait()
                load_two(layer, blk).wait()
                for which in range(2):
                    for r0 in range(0, FB, 64):
                        rows = pl.ds(r0, 64)
                        wlo[layer, blk, which, rows] = wgt[layer, blk, which, rows].astype(BF16)
            else:
                combine(step - 1, layer, blk, True)

            w_one = wlo[layer, blk, 0]
            w_two = wlo[layer, blk, 1]
            for r in range(NR):
                rows = pl.ds(r * RT, RT)
                z = dot_nn(nlo[layer, rows], w_one)
                pre[layer, blk, rows] = z
                th = jnp.tanh(z * (GELU_C + (GELU_C * GELU_K) * (z * z)))
                a_lo = (z * (0.5 + 0.5 * th)).astype(BF16)
                act[layer, blk, rows] = a_lo
                acc[rows] = acc[rows] + dot_nn(a_lo, w_two)

    def backward_layer(step, layer, send_now):
        if layer > 0:
            @pl.loop(0, BATCH, step=128)
            def _(r0):
                rows = pl.ds(pl.multiple_of(r0, 128), 128)
                macc[rows] = jnp.zeros((128, DM), F32)

        @pl.loop(0, NB)
        def _(blk):
            @pl.when(step > 0)
            def _():
                wait_sends(step - 1, layer, blk)

            g_two = dot_tn(act[layer, blk], elo[...])
            q_two = wgt[layer, blk, 1] - LEARN_RATE * g_two
            wgt[layer, blk, 1] = q_two
            wire[layer, blk, 1] = q_two.astype(BF16)
            w_one = wlo[layer, blk, 0]
            w_two = wlo[layer, blk, 1]
            for r in range(NR):
                rows = pl.ds(r * RT, RT)
                u = dot_nt(elo[rows], w_two)
                z = pre[layer, blk, rows]
                zz = z * z
                th = jnp.tanh(z * (GELU_C + (GELU_C * GELU_K) * zz))
                slope = (0.5 + 0.5 * th) * (1.0 + (z * (1.0 - th)) * (GELU_C + (3.0 * GELU_C * GELU_K) * zz))
                dz = (u * slope).astype(BF16)
                dzb[rows] = dz
                if layer > 0:
                    macc[rows] = macc[rows] + dot_nt(dz, w_one)
            g_one = dot_tn(nlo[layer], dzb[...])
            q_one = wgt[layer, blk, 0] - LEARN_RATE * g_one
            wgt[layer, blk, 0] = q_one
            wire[layer, blk, 0] = q_one.astype(BF16)
            send_now(blk)

    def forward(step, first):
        load_a(step).wait()
        with jax.named_scope("fwd0"):
            forward_layer(step, 0, first)
        with jax.named_scope("fwd1"):
            forward_layer(step, 1, first)

    forward(0, True)
    pl.semaphore_wait(barrier, n_rows + 1)

    @pl.loop(0, STEPS)
    def _(step):
        load_t(step).wait()

        @pl.loop(0, BATCH, step=128)
        def _(r0):
            rows = pl.ds(pl.multiple_of(r0, 128), 128)
            e = (2.0 / (BATCH * DM)) * (acc[rows].astype(BF16).astype(F32) - tin[step, rows].astype(F32))
            err[rows] = e
            elo[rows] = e.astype(BF16)

        def send_first(blk):
            @pl.when(blk < EARLY)
            def _():
                start_sends(step, 1, blk)

        backward_layer(step, 1, send_first)

        @pl.loop(0, BATCH, step=128)
        def _(r0):
            rows = pl.ds(pl.multiple_of(r0, 128), 128)
            m = macc[rows]
            n = nf1[rows]
            inv = inv1[rows, 0:1]
            e = err[rows] + inv * (m - n * jnp.mean(m * n, axis=-1, keepdims=True))
            elo[rows] = e.astype(BF16)

        backward_layer(step, 0, lambda blk: start_sends(step, 0, blk))
        for blk in range(EARLY, NB):
            start_sends(step, 1, blk)
        start_outward(step)

        @pl.when(step < STEPS - 1)
        def _():
            forward(step + 1, False)

    for layer, blk in SEND_ORDER:
        combine(STEPS - 1, layer, blk, False)
    for layer, blk in SEND_ORDER:
        wait_sends(STEPS - 1, layer, blk)

        @pl.when(inner)
        def _():
            relay(STEPS - 1, layer, blk).wait_send()


def store_kernel(wgt, o1_hbm, o2_hbm, out_sem):
    copies = []
    for layer in range(LAYERS):
        for blk in range(NB):
            span = pl.ds(blk * FB, FB)
            copies.append(pltpu.make_async_copy(wgt.at[layer, blk, 0], o1_hbm.at[layer, :, span], out_sem.at[layer, blk, 0]))
            copies.append(pltpu.make_async_copy(wgt.at[layer, blk, 1], o2_hbm.at[layer, span, :], out_sem.at[layer, blk, 1]))
    for copy in copies:
        copy.start()
    for copy in copies:
        copy.wait()


def solution(mesh):
    n_rows = mesh.shape["row"]
    n_cols = mesh.shape["col"]

    def device_fn(w_one, w_two, inputs, targets):
        chunk = (LAYERS, NB, 2, FB, DM)
        weights = pl.pallas_call(
            functools.partial(kernel, n_rows, n_cols),
            out_shape=pltpu.VMEM(chunk, F32),
            in_specs=[pl.BlockSpec(memory_space=pl.ANY)] * 4,
            out_specs=pl.BlockSpec(memory_space=pltpu.VMEM),
            scratch_shapes=[
                pltpu.VMEM(chunk, BF16),
                pltpu.VMEM(chunk, BF16),
                pltpu.VMEM((STEPS, 4) + chunk, BF16),
                pltpu.VMEM((STEPS, BATCH, DM), BF16),
                pltpu.VMEM((STEPS, BATCH, DM), BF16),
                pltpu.VMEM((LAYERS, BATCH, DM), BF16),
                pltpu.VMEM((BATCH, DM), F32),
                pltpu.VMEM((BATCH, 128), F32),
                pltpu.VMEM((LAYERS, NB, BATCH, FB), BF16),
                pltpu.VMEM((LAYERS, NB, BATCH, FB), F32),
                pltpu.VMEM((BATCH, DM), F32),
                pltpu.VMEM((BATCH, DM), F32),
                pltpu.VMEM((BATCH, DM), BF16),
                pltpu.VMEM((BATCH, FB), BF16),
                pltpu.VMEM((BATCH, DM), F32),
                pltpu.SemaphoreType.DMA((LAYERS, NB, 2)),
                pltpu.SemaphoreType.DMA((2, STEPS)),
                pltpu.SemaphoreType.DMA((4, LAYERS, NB)),
                pltpu.SemaphoreType.DMA((STEPS, 4, LAYERS, NB)),
                pltpu.SemaphoreType.DMA((LAYERS, NB)),
            ],
            compiler_params=pltpu.CompilerParams(
                collective_id=0, has_side_effects=True, vmem_limit_bytes=58 * 2**20),
        )(w_one[0, 0], w_two[0, 0], inputs[0, 0], targets[0, 0])
        out_one, out_two = pl.pallas_call(
            store_kernel,
            out_shape=[
                jax.ShapeDtypeStruct((LAYERS, DM, DF), F32),
                jax.ShapeDtypeStruct((LAYERS, DF, DM), F32),
            ],
            in_specs=[pl.BlockSpec(memory_space=pltpu.VMEM)],
            out_specs=[pl.BlockSpec(memory_space=pl.ANY)] * 2,
            scratch_shapes=[pltpu.SemaphoreType.DMA((LAYERS, NB, 2))],
            compiler_params=pltpu.CompilerParams(vmem_limit_bytes=2**20),
        )(weights)
        return out_one[None, None], out_two[None, None]

    grid_spec = P("row", "col")
    return jax.shard_map(device_fn, mesh=mesh, in_specs=(grid_spec,) * 4, out_specs=(grid_spec,) * 2, check_vma=False)
```

```python
import functools

import jax
import jax.numpy as jnp
from jax import lax
from jax.experimental import pallas as pl
from jax.experimental.pallas import tpu as pltpu
from jax.sharding import PartitionSpec as P

LEARN_RATE = 1.5
NORM_EPS = 1e-6
GELU_C = 0.7978845608028654
GELU_K = 0.044715

STEPS = 3
LAYERS = 2
BATCH = 1024
DM = 256
DF = 1024
FB = 256
NB = DF // FB
RT = 256
NR = BATCH // RT
MESH = pl.DeviceIdType.MESH
F32 = jnp.float32
BF16 = jnp.bfloat16

EARLY = 2
SEND_ORDER = [(1, b) for b in range(EARLY)] + [(0, b) for b in range(NB)] + [(1, b) for b in range(EARLY, NB)]


def dot_nn(a, b):
    return lax.dot_general(a, b, (((1,), (0,)), ((), ())), preferred_element_type=F32)


def dot_nt(a, b):
    return lax.dot_general(a, b, (((1,), (1,)), ((), ())), preferred_element_type=F32)


def dot_tn(a, b):
    return lax.dot_general(a, b, (((0,), (0,)), ((), ())), preferred_element_type=F32)


def kernel(n_rows, n_cols, w1_hbm, w2_hbm, a_hbm, t_hbm, wgt,
           wlo, wire, recv, ain, tin, nlo, nf1, inv1, act, pre, acc, err, elo, dzb, macc,
           load_sem, data_sem, send_sem, recv_sem, relay_sem):
    row = lax.axis_index("row")
    col = lax.axis_index("col")
    half = row // 2
    inner = jnp.logical_and(row > 0, row < n_rows - 1)
    targets = (
        ((row, lax.rem(col + 1, n_cols)), 0),
        ((row, lax.rem(col + n_cols - 1, n_cols)), 1),
        ((row + 1 - 2 * half, col), lax.rem(row + half, 2) * -1 + 3),
        ((row - 1 + 2 * half, col), 2),
    )
    relay_device = (3 - 3 * half, col)

    def load_one(layer, blk):
        return pltpu.make_async_copy(
            w1_hbm.at[layer, :, pl.ds(pl.multiple_of(blk * FB, FB), FB)], wgt.at[layer, blk, 0], load_sem.at[layer, blk])

    def load_two(layer, blk):
        return pltpu.make_async_copy(
            w2_hbm.at[layer, pl.ds(pl.multiple_of(blk * FB, FB), FB), :], wgt.at[layer, blk, 1], load_sem.at[layer, blk])

    def loaded(layer, blk):
        return pltpu.make_async_copy(wgt.at[layer, blk], wgt.at[layer, blk], load_sem.at[layer, blk])

    def load_data(which, first, count):
        src, dst = ((a_hbm, ain), (t_hbm, tin))[which]
        return pltpu.make_async_copy(src.at[pl.ds(first, count)], dst.at[pl.ds(first, count)], data_sem.at[which, min(first, 1)])

    load_data(0, 0, 1).start()

    @pl.loop(0, LAYERS * NB)
    def _(i):
        load_one(i // NB, lax.rem(i, NB)).start()
        load_two(i // NB, lax.rem(i, NB)).start()

    barrier = pltpu.get_barrier_semaphore()
    for shift in range(1, n_rows):
        pl.semaphore_signal(barrier, inc=1, device_id=(lax.rem(row + shift, n_rows), col), device_id_type=MESH)
    for tgt, _ in targets[:2]:
        pl.semaphore_signal(barrier, inc=1, device_id=tgt, device_id_type=MESH)
    load_data(1, 0, 1).start()
    load_data(0, 1, STEPS - 1).start()
    load_data(1, 1, STEPS - 1).start()

    def remote(src, dst, sent, arrived, device):
        return pltpu.make_async_remote_copy(
            src_ref=src, dst_ref=dst, send_sem=sent, recv_sem=arrived, device_id=device, device_id_type=MESH)

    def send(step, kind, layer, *blk):
        device, slot = targets[kind]
        group = slot - 2 if kind == 2 else 0
        return remote(
            wire.at[(layer,) + blk], recv.at[(step, slot, layer) + blk],
            send_sem.at[kind], recv_sem.at[lax.rem(step, 2), group, layer, blk[0]], device)

    def relay(step, layer, blk):
        return remote(
            recv.at[step, 3, layer, blk], recv.at[step, 3, layer, blk],
            relay_sem.at[0], recv_sem.at[lax.rem(step, 2), 1, layer, blk], relay_device)

    def wait_far(step, layer, blk):
        relay(step, layer, blk).wait_recv()

    def wait_rest(step, layer, blk):
        dst = recv.at[step, pl.ds(0, 3), layer, blk]
        remote(dst, dst, send_sem.at[0], recv_sem.at[lax.rem(step, 2), 0, layer, blk], relay_device).wait_recv()

    def wait_relays(step):
        remote(recv.at[step, 3], recv.at[step, 3], relay_sem.at[0], recv_sem.at[0, 0, 0, 0], relay_device).wait_send()

    def start_sends(step, layer, *blk):
        send(step, 2, layer, *blk).start()

        @pl.when(jnp.logical_and(inner, step == 0))
        def _():
            send(step, 3, layer, *blk).start()
        for kind in (0, 1):
            send(step, kind, layer, *blk).start()

    def start_outward(step):
        @pl.when(jnp.logical_and(inner, step > 0))
        def _():
            wait_relays(step - 1)
            for layer, blk in SEND_ORDER:
                send(step, 3, layer, blk).start()

    def wait_sends():
        for kind in range(3):
            remote(wire, recv.at[0, 0], send_sem.at[kind], recv_sem.at[0, 0, 0, 0], relay_device).wait_send()

        @pl.when(inner)
        def _():
            remote(wire, recv.at[0, 0], send_sem.at[3], recv_sem.at[0, 0, 0, 0], relay_device).wait_send()

    def combine(step, layer, blk, keep_lo):
        with jax.named_scope("w_far"):
            wait_far(step, layer, blk)

        @pl.when(inner)
        def _():
            relay(step, layer, blk).start()
        with jax.named_scope("w_rest"):
            wait_rest(step, layer, blk)
        for which in range(2):
            @pl.loop(0, FB, step=64)
            def _(r0):
                rows = pl.ds(pl.multiple_of(r0, 64), 64)
                tot = wgt[layer, blk, which, rows]
                for slot in (0, 1, 3 - half, 2 + half):
                    tot = tot + recv[step, slot, layer, blk, which, rows].astype(F32)
                tot = tot * 0.2
                wgt[layer, blk, which, rows] = tot
                if keep_lo:
                    wlo[layer, blk, which, rows] = tot.astype(BF16)

    def normalise(step, layer):
        for r0 in range(0, BATCH, 128):
            rows = pl.ds(r0, 128)
            if layer == 0:
                x = ain[step, rows].astype(F32)
            else:
                x = acc[rows].astype(BF16).astype(F32)
            inv = lax.rsqrt(jnp.mean(x * x, axis=-1, keepdims=True) + NORM_EPS)
            n = x * inv
            nlo[layer, rows] = n.astype(BF16)
            if layer == 1:
                nf1[rows] = n
                inv1[rows] = jnp.broadcast_to(inv, (128, 128))
            acc[rows] = x

    def forward_layer(step, layer, first):
        normalise(step, layer)

        def block(blk):
            if first:
                loaded(layer, blk).wait()
                for which in range(2):
                    for r0 in range(0, FB, 64):
                        rows = pl.ds(r0, 64)
                        wlo[layer, blk, which, rows] = wgt[layer, blk, which, rows].astype(BF16)
            else:
                combine(step - 1, layer, blk, True)

            w_one = wlo[layer, blk, 0]
            w_two = wlo[layer, blk, 1]
            for r in range(NR):
                rows = pl.ds(r * RT, RT)
                z = dot_nn(nlo[layer, rows], w_one)
                pre[layer, blk, rows] = z
                th = jnp.tanh(z * (GELU_C + (GELU_C * GELU_K) * (z * z)))
                a_lo = (z * (0.5 + 0.5 * th)).astype(BF16)
                act[layer, blk, rows] = a_lo
                acc[rows] = acc[rows] + dot_nn(a_lo, w_two)

        if first:
            for blk in range(NB):
                block(blk)
        else:
            pl.loop(0, NB)(block)

    def backward_layer(step, layer, send_now):
        if layer > 0:
            @pl.loop(0, BATCH, step=128)
            def _(r0):
                rows = pl.ds(pl.multiple_of(r0, 128), 128)
                macc[rows] = jnp.zeros((128, DM), F32)

        @pl.loop(0, NB)
        def _(blk):
            g_two = dot_tn(act[layer, blk], elo[...])
            q_two = wgt[layer, blk, 1] - LEARN_RATE * g_two
            wgt[layer, blk, 1] = q_two
            wire[layer, blk, 1] = q_two.astype(BF16)
            send_now(blk, 1)
            w_one = wlo[layer, blk, 0]
            w_two = wlo[layer, blk, 1]
            for r in range(NR):
                rows = pl.ds(r * RT, RT)
                u = dot_nt(elo[rows], w_two)
                z = pre[layer, blk, rows]
                zz = z * z
                th = jnp.tanh(z * (GELU_C + (GELU_C * GELU_K) * zz))
                slope = (0.5 + 0.5 * th) * (1.0 + (z * (1.0 - th)) * (GELU_C + (3.0 * GELU_C * GELU_K) * zz))
                dz = (u * slope).astype(BF16)
                dzb[rows] = dz
                if layer > 0:
                    macc[rows] = macc[rows] + dot_nt(dz, w_one)
            g_one = dot_tn(nlo[layer], dzb[...])
            q_one = wgt[layer, blk, 0] - LEARN_RATE * g_one
            wgt[layer, blk, 0] = q_one
            wire[layer, blk, 0] = q_one.astype(BF16)
            send_now(blk, 0)

    def forward(step, first):
        with jax.named_scope("fwd0"):
            forward_layer(step, 0, first)
        with jax.named_scope("fwd1"):
            forward_layer(step, 1, first)

    load_data(0, 0, 1).wait()
    forward(0, True)
    pl.semaphore_wait(barrier, n_rows + 1)

    load_data(1, 0, 1).wait()

    @pl.loop(0, STEPS)
    def _(step):

        @pl.loop(0, BATCH, step=128)
        def _(r0):
            rows = pl.ds(pl.multiple_of(r0, 128), 128)
            e = (2.0 / (BATCH * DM)) * (acc[rows].astype(BF16).astype(F32) - tin[step, rows].astype(F32))
            err[rows] = e
            elo[rows] = e.astype(BF16)

        @pl.when(step > 0)
        def _():
            wait_sends()

        def send_early(blk, which):
            @pl.when(blk < EARLY)
            def _():
                start_sends(step, 1, blk, which)

        with jax.named_scope("bwd1"):
            backward_layer(step, 1, send_early)

        @pl.loop(0, BATCH, step=128)
        def _(r0):
            rows = pl.ds(pl.multiple_of(r0, 128), 128)
            m = macc[rows]
            n = nf1[rows]
            inv = inv1[rows, 0:1]
            e = err[rows] + inv * (m - n * jnp.mean(m * n, axis=-1, keepdims=True))
            elo[rows] = e.astype(BF16)

        def send_whole(blk, which):
            if which == 0:
                start_sends(step, 0, blk)

        with jax.named_scope("bwd0"):
            backward_layer(step, 0, send_whole)
        for blk in range(EARLY, NB):
            start_sends(step, 1, blk)
        with jax.named_scope("outward"):
            start_outward(step)

        @pl.when(step == 0)
        def _():
            load_data(0, 1, STEPS - 1).wait()
            load_data(1, 1, STEPS - 1).wait()

        @pl.when(step < STEPS - 1)
        def _():
            forward(step + 1, False)

    for layer, blk in SEND_ORDER:
        combine(STEPS - 1, layer, blk, False)
    wait_sends()

    @pl.when(inner)
    def _():
        wait_relays(STEPS - 1)


def store_kernel(wgt, o1_hbm, o2_hbm, out_sem):
    copies = []
    for layer in range(LAYERS):
        for blk in range(NB):
            span = pl.ds(blk * FB, FB)
            copies.append(pltpu.make_async_copy(wgt.at[layer, blk, 0], o1_hbm.at[layer, :, span], out_sem.at[layer, blk, 0]))
            copies.append(pltpu.make_async_copy(wgt.at[layer, blk, 1], o2_hbm.at[layer, span, :], out_sem.at[layer, blk, 1]))
    for copy in copies:
        copy.start()
    for copy in copies:
        copy.wait()


def solution(mesh):
    n_rows = mesh.shape["row"]
    n_cols = mesh.shape["col"]

    def device_fn(w_one, w_two, inputs, targets):
        chunk = (LAYERS, NB, 2, FB, DM)
        weights = pl.pallas_call(
            functools.partial(kernel, n_rows, n_cols),
            out_shape=pltpu.VMEM(chunk, F32),
            in_specs=[pl.BlockSpec(memory_space=pl.ANY)] * 4,
            out_specs=pl.BlockSpec(memory_space=pltpu.VMEM),
            scratch_shapes=[
                pltpu.VMEM(chunk, BF16),
                pltpu.VMEM(chunk, BF16),
                pltpu.VMEM((STEPS, 4) + chunk, BF16),
                pltpu.VMEM((STEPS, BATCH, DM), BF16),
                pltpu.VMEM((STEPS, BATCH, DM), BF16),
                pltpu.VMEM((LAYERS, BATCH, DM), BF16),
                pltpu.VMEM((BATCH, DM), F32),
                pltpu.VMEM((BATCH, 128), F32),
                pltpu.VMEM((LAYERS, NB, BATCH, FB), BF16),
                pltpu.VMEM((LAYERS, NB, BATCH, FB), F32),
                pltpu.VMEM((BATCH, DM), F32),
                pltpu.VMEM((BATCH, DM), F32),
                pltpu.VMEM((BATCH, DM), BF16),
                pltpu.VMEM((BATCH, FB), BF16),
                pltpu.VMEM((BATCH, DM), F32),
                pltpu.SemaphoreType.DMA((LAYERS, NB)),
                pltpu.SemaphoreType.DMA((2, 2)),
                pltpu.SemaphoreType.DMA((4,)),
                pltpu.SemaphoreType.DMA((2, 2, LAYERS, NB)),
                pltpu.SemaphoreType.DMA((1,)),
            ],
            compiler_params=pltpu.CompilerParams(
                collective_id=0, has_side_effects=True, vmem_limit_bytes=58 * 2**20),
        )(w_one[0, 0], w_two[0, 0], inputs[0, 0], targets[0, 0])
        out_one, out_two = pl.pallas_call(
            store_kernel,
            out_shape=[
                jax.ShapeDtypeStruct((LAYERS, DM, DF), F32),
                jax.ShapeDtypeStruct((LAYERS, DF, DM), F32),
            ],
            in_specs=[pl.BlockSpec(memory_space=pltpu.VMEM)],
            out_specs=[pl.BlockSpec(memory_space=pl.ANY)] * 2,
            scratch_shapes=[pltpu.SemaphoreType.DMA((LAYERS, NB, 2))],
            compiler_params=pltpu.CompilerParams(vmem_limit_bytes=2**20),
        )(weights)
        return out_one[None, None], out_two[None, None]

    grid_spec = P("row", "col")
    return jax.shard_map(device_fn, mesh=mesh, in_specs=(grid_spec,) * 4, out_specs=(grid_spec,) * 2, check_vma=False)
```

```python
import functools

import jax
import jax.numpy as jnp
from jax import lax
from jax.experimental import pallas as pl
from jax.experimental.pallas import tpu as pltpu
from jax.sharding import PartitionSpec as P

LEARN_RATE = 1.5
NORM_EPS = 1e-6
GELU_C = 0.7978845608028654
GELU_K = 0.044715

STEPS = 3
LAYERS = 2
BATCH = 1024
DM = 256
DF = 1024
FB = 256
NB = DF // FB
RT = 256
NR = BATCH // RT
RT1 = 256
MESH = pl.DeviceIdType.MESH
F32 = jnp.float32
BF16 = jnp.bfloat16

EARLY = 2
SEND_ORDER = [(1, b) for b in range(EARLY)] + [(0, b) for b in range(NB)] + [(1, b) for b in range(EARLY, NB)]


def dot_nn(a, b):
    return lax.dot_general(a, b, (((1,), (0,)), ((), ())), preferred_element_type=F32)


def dot_nt(a, b):
    return lax.dot_general(a, b, (((1,), (1,)), ((), ())), preferred_element_type=F32)


def dot_tn(a, b):
    return lax.dot_general(a, b, (((0,), (0,)), ((), ())), preferred_element_type=F32)


def kernel(n_rows, n_cols, w1_hbm, w2_hbm, a_hbm, t_hbm, wgt,
           wlo, wire, recv, ain, tin, nlo, nf1, inv1, act, acc, err, elo, dzb, macc,
           load_sem, data_sem, send_sem, recv_sem, relay_sem):
    row = lax.axis_index("row")
    col = lax.axis_index("col")
    half = row // 2
    inner = jnp.logical_and(row > 0, row < n_rows - 1)
    targets = (
        ((row, lax.rem(col + 1, n_cols)), 0),
        ((row, lax.rem(col + n_cols - 1, n_cols)), 1),
        ((row + 1 - 2 * half, col), lax.rem(row + half, 2) * -1 + 3),
        ((row - 1 + 2 * half, col), 2),
    )
    relay_device = (3 - 3 * half, col)

    def load_one(layer, blk):
        return pltpu.make_async_copy(
            w1_hbm.at[layer, :, pl.ds(pl.multiple_of(blk * FB, FB), FB)], wgt.at[layer, blk, 0], load_sem.at[layer, blk])

    def load_two(layer, blk):
        return pltpu.make_async_copy(
            w2_hbm.at[layer, pl.ds(pl.multiple_of(blk * FB, FB), FB), :], wgt.at[layer, blk, 1], load_sem.at[layer, blk])

    def loaded(layer, blk):
        return pltpu.make_async_copy(wgt.at[layer, blk], wgt.at[layer, blk], load_sem.at[layer, blk])

    def load_data(which, first, count):
        src, dst = ((a_hbm, ain), (t_hbm, tin))[which]
        return pltpu.make_async_copy(src.at[pl.ds(first, count)], dst.at[pl.ds(first, count)], data_sem.at[which, min(first, 1)])

    load_data(0, 0, 1).start()

    @pl.loop(0, LAYERS * NB)
    def _(i):
        load_one(i // NB, lax.rem(i, NB)).start()
        load_two(i // NB, lax.rem(i, NB)).start()

    barrier = pltpu.get_barrier_semaphore()
    for shift in range(1, n_rows):
        pl.semaphore_signal(barrier, inc=1, device_id=(lax.rem(row + shift, n_rows), col), device_id_type=MESH)
    for tgt, _ in targets[:2]:
        pl.semaphore_signal(barrier, inc=1, device_id=tgt, device_id_type=MESH)
    load_data(1, 0, 1).start()
    load_data(0, 1, STEPS - 1).start()
    load_data(1, 1, STEPS - 1).start()

    def remote(src, dst, sent, arrived, device):
        return pltpu.make_async_remote_copy(
            src_ref=src, dst_ref=dst, send_sem=sent, recv_sem=arrived, device_id=device, device_id_type=MESH)

    def send(step, kind, layer, *blk):
        device, slot = targets[kind]
        group = slot - 2 if kind == 2 else 0
        return remote(
            wire.at[(layer,) + blk], recv.at[(step, slot, layer) + blk],
            send_sem.at[kind], recv_sem.at[lax.rem(step, 2), group, layer, blk[0]], device)

    def relay(step, layer, blk):
        return remote(
            recv.at[step, 3, layer, blk], recv.at[step, 3, layer, blk],
            relay_sem.at[0], recv_sem.at[lax.rem(step, 2), 1, layer, blk], relay_device)

    def wait_far(step, layer, blk):
        relay(step, layer, blk).wait_recv()

    def wait_rest(step, layer, blk):
        dst = recv.at[step, pl.ds(0, 3), layer, blk]
        remote(dst, dst, send_sem.at[0], recv_sem.at[lax.rem(step, 2), 0, layer, blk], relay_device).wait_recv()

    def wait_relays(step):
        remote(recv.at[step, 3], recv.at[step, 3], relay_sem.at[0], recv_sem.at[0, 0, 0, 0], relay_device).wait_send()

    def start_sends(step, layer, *blk, hold=False):
        if hold:
            @pl.when(jnp.logical_not(jnp.logical_and(inner, step == STEPS - 1)))
            def _():
                send(step, 2, layer, *blk).start()
        else:
            send(step, 2, layer, *blk).start()

        @pl.when(jnp.logical_and(inner, step == 0))
        def _():
            send(step, 3, layer, *blk).start()
        for kind in (0, 1):
            send(step, kind, layer, *blk).start()

    def start_outward(step):
        @pl.when(jnp.logical_and(inner, step > 0))
        def _():
            wait_relays(step - 1)
            for layer, blk in SEND_ORDER:
                send(step, 3, layer, blk).start()

    def wait_sends():
        for kind in range(3):
            remote(wire, recv.at[0, 0], send_sem.at[kind], recv_sem.at[0, 0, 0, 0], relay_device).wait_send()

        @pl.when(inner)
        def _():
            remote(wire, recv.at[0, 0], send_sem.at[3], recv_sem.at[0, 0, 0, 0], relay_device).wait_send()

    def combine(step, layer, blk, keep_lo, held_back=False):
        with jax.named_scope("w_far"):
            wait_far(step, layer, blk)

        @pl.when(inner)
        def _():
            relay(step, layer, blk).start()
        if held_back:
            @pl.when(inner)
            def _():
                send(step, 2, layer, blk).start()
        with jax.named_scope("w_rest"):
            wait_rest(step, layer, blk)
        for which in range(2):
            @pl.loop(0, FB, step=64)
            def _(r0):
                rows = pl.ds(pl.multiple_of(r0, 64), 64)
                tot = wgt[layer, blk, which, rows]
                for slot in (0, 1, 3 - half, 2 + half):
                    tot = tot + recv[step, slot, layer, blk, which, rows].astype(F32)
                tot = tot * 0.2
                wgt[layer, blk, which, rows] = tot
                if keep_lo:
                    wlo[layer, blk, which, rows] = tot.astype(BF16)

    def normalise(layer, rows, x):
        inv = lax.rsqrt(jnp.mean(x * x, axis=-1, keepdims=True) + NORM_EPS)
        n = x * inv
        nlo[layer, rows] = n.astype(BF16)
        if layer == 1:
            nf1[rows] = n
            inv1[rows] = jnp.broadcast_to(inv, (x.shape[0], 128))

    def activation(layer, blk, rows):
        z = dot_nn(nlo[layer, rows], wlo[layer, blk, 0])
        th = jnp.tanh(z * (GELU_C + (GELU_C * GELU_K) * (z * z)))
        a_lo = (z * (0.5 + 0.5 * th)).astype(BF16)
        act[layer, blk, rows] = a_lo
        return a_lo

    def error(step, rows, total):
        e = (2.0 / (BATCH * DM)) * (total.astype(BF16).astype(F32) - tin[step, rows].astype(F32))
        err[rows] = e
        elo[rows] = e.astype(BF16)

    def first_forward():
        load_data(0, 0, 1).wait()
        for layer in range(LAYERS):
            if layer == LAYERS - 1:
                load_data(1, 0, 1).wait()
            for r in range(BATCH // RT1):
                rows = pl.ds(r * RT1, RT1)
                if layer == 0:
                    total = ain[0, rows].astype(F32)
                    normalise(layer, rows, total)
                else:
                    total = acc[rows]
                for blk in range(NB):
                    if r == 0:
                        loaded(layer, blk).wait()
                        wlo[layer, blk] = wgt[layer, blk].astype(BF16)
                    total = total + dot_nn(activation(layer, blk, rows), wlo[layer, blk, 1])
                if layer == 0:
                    total = total.astype(BF16).astype(F32)
                    normalise(1, rows, total)
                    acc[rows] = total
                else:
                    error(0, rows, total)

    def forward_layer(step, layer):
        for r0 in range(0, BATCH, 128):
            rows = pl.ds(r0, 128)
            x = ain[step, rows].astype(F32) if layer == 0 else acc[rows].astype(BF16).astype(F32)
            normalise(layer, rows, x)
            acc[rows] = x

        @pl.loop(0, NB)
        def _(blk):
            combine(step - 1, layer, blk, True)
            for r in range(NR):
                rows = pl.ds(r * RT, RT)
                acc[rows] = acc[rows] + dot_nn(activation(layer, blk, rows), wlo[layer, blk, 1])

    def backward_layer(step, layer, send_now):
        if layer > 0:
            @pl.loop(0, BATCH, step=128)
            def _(r0):
                rows = pl.ds(pl.multiple_of(r0, 128), 128)
                macc[rows] = jnp.zeros((128, DM), F32)

        @pl.loop(0, NB)
        def _(blk):
            g_two = dot_tn(act[layer, blk], elo[...])
            q_two = wgt[layer, blk, 1] - LEARN_RATE * g_two
            wgt[layer, blk, 1] = q_two
            wire[layer, blk, 1] = q_two.astype(BF16)
            send_now(blk, 1)
            w_one = wlo[layer, blk, 0]
            w_two = wlo[layer, blk, 1]
            for r in range(NR):
                rows = pl.ds(r * RT, RT)
                u = dot_nt(elo[rows], w_two)
                z = dot_nn(nlo[layer, rows], w_one)
                zz = z * z
                th = jnp.tanh(z * (GELU_C + (GELU_C * GELU_K) * zz))
                slope = (0.5 + 0.5 * th) * (1.0 + (z * (1.0 - th)) * (GELU_C + (3.0 * GELU_C * GELU_K) * zz))
                dz = (u * slope).astype(BF16)
                dzb[rows] = dz
                if layer > 0:
                    macc[rows] = macc[rows] + dot_nt(dz, w_one)
            g_one = dot_tn(nlo[layer], dzb[...])
            q_one = wgt[layer, blk, 0] - LEARN_RATE * g_one
            wgt[layer, blk, 0] = q_one
            wire[layer, blk, 0] = q_one.astype(BF16)
            send_now(blk, 0)

    with jax.named_scope("fwd_first"):
        first_forward()
    pl.semaphore_wait(barrier, n_rows + 1)

    @pl.loop(0, STEPS)
    def _(step):
        @pl.when(step > 0)
        def _():
            wait_sends()

        def send_early(blk, which):
            @pl.when(blk < EARLY)
            def _():
                start_sends(step, 1, blk, which)

        with jax.named_scope("bwd1"):
            backward_layer(step, 1, send_early)

        @pl.loop(0, BATCH, step=128)
        def _(r0):
            rows = pl.ds(pl.multiple_of(r0, 128), 128)
            m = macc[rows]
            n = nf1[rows]
            inv = inv1[rows, 0:1]
            e = err[rows] + inv * (m - n * jnp.mean(m * n, axis=-1, keepdims=True))
            elo[rows] = e.astype(BF16)

        def send_whole(blk, which):
            if which == 0:
                start_sends(step, 0, blk)

        with jax.named_scope("bwd0"):
            backward_layer(step, 0, send_whole)
        for blk in range(EARLY, NB):
            start_sends(step, 1, blk, hold=(1, blk) == SEND_ORDER[-1])
        with jax.named_scope("outward"):
            start_outward(step)

        @pl.when(step == 0)
        def _():
            load_data(0, 1, STEPS - 1).wait()
            load_data(1, 1, STEPS - 1).wait()

        @pl.when(step < STEPS - 1)
        def _():
            with jax.named_scope("fwd0"):
                forward_layer(step + 1, 0)
            with jax.named_scope("fwd1"):
                forward_layer(step + 1, 1)
            for r0 in range(0, BATCH, 128):
                error(step + 1, pl.ds(r0, 128), acc[pl.ds(r0, 128)])

    for layer, blk in SEND_ORDER:
        combine(STEPS - 1, layer, blk, False, held_back=(layer, blk) == SEND_ORDER[-1])
    wait_sends()

    @pl.when(inner)
    def _():
        wait_relays(STEPS - 1)


def store_kernel(wgt, o1_hbm, o2_hbm, out_sem):
    copies = []
    for layer in range(LAYERS):
        for blk in range(NB):
            span = pl.ds(blk * FB, FB)
            copies.append(pltpu.make_async_copy(wgt.at[layer, blk, 0], o1_hbm.at[layer, :, span], out_sem.at[layer, blk, 0]))
            copies.append(pltpu.make_async_copy(wgt.at[layer, blk, 1], o2_hbm.at[layer, span, :], out_sem.at[layer, blk, 1]))
    for copy in copies:
        copy.start()
    for copy in copies:
        copy.wait()


def solution(mesh):
    n_rows = mesh.shape["row"]
    n_cols = mesh.shape["col"]

    def device_fn(w_one, w_two, inputs, targets):
        chunk = (LAYERS, NB, 2, FB, DM)
        weights = pl.pallas_call(
            functools.partial(kernel, n_rows, n_cols),
            out_shape=pltpu.VMEM(chunk, F32),
            in_specs=[pl.BlockSpec(memory_space=pl.ANY)] * 4,
            out_specs=pl.BlockSpec(memory_space=pltpu.VMEM),
            scratch_shapes=[
                pltpu.VMEM(chunk, BF16),
                pltpu.VMEM(chunk, BF16),
                pltpu.VMEM((STEPS, 4) + chunk, BF16),
                pltpu.VMEM((STEPS, BATCH, DM), BF16),
                pltpu.VMEM((STEPS, BATCH, DM), BF16),
                pltpu.VMEM((LAYERS, BATCH, DM), BF16),
                pltpu.VMEM((BATCH, DM), F32),
                pltpu.VMEM((BATCH, 128), F32),
                pltpu.VMEM((LAYERS, NB, BATCH, FB), BF16),
                pltpu.VMEM((BATCH, DM), F32),
                pltpu.VMEM((BATCH, DM), F32),
                pltpu.VMEM((BATCH, DM), BF16),
                pltpu.VMEM((BATCH, FB), BF16),
                pltpu.VMEM((BATCH, DM), F32),
                pltpu.SemaphoreType.DMA((LAYERS, NB)),
                pltpu.SemaphoreType.DMA((2, 2)),
                pltpu.SemaphoreType.DMA((4,)),
                pltpu.SemaphoreType.DMA((2, 2, LAYERS, NB)),
                pltpu.SemaphoreType.DMA((1,)),
            ],
            compiler_params=pltpu.CompilerParams(
                collective_id=0, has_side_effects=True, vmem_limit_bytes=58 * 2**20),
        )(w_one[0, 0], w_two[0, 0], inputs[0, 0], targets[0, 0])
        out_one, out_two = pl.pallas_call(
            store_kernel,
            out_shape=[
                jax.ShapeDtypeStruct((LAYERS, DM, DF), F32),
                jax.ShapeDtypeStruct((LAYERS, DF, DM), F32),
            ],
            in_specs=[pl.BlockSpec(memory_space=pltpu.VMEM)],
            out_specs=[pl.BlockSpec(memory_space=pl.ANY)] * 2,
            scratch_shapes=[pltpu.SemaphoreType.DMA((LAYERS, NB, 2))],
            compiler_params=pltpu.CompilerParams(vmem_limit_bytes=2**20),
        )(weights)
        return out_one[None, None], out_two[None, None]

    grid_spec = P("row", "col")
    return jax.shard_map(device_fn, mesh=mesh, in_specs=(grid_spec,) * 4, out_specs=(grid_spec,) * 2, check_vma=False)
```

```python
import functools

import jax
import jax.numpy as jnp
from jax import lax
from jax.experimental import pallas as pl
from jax.experimental.pallas import tpu as pltpu
from jax.sharding import PartitionSpec as P

LEARN_RATE = 1.5
NORM_EPS = 1e-6
GELU_C = 0.7978845608028654
GELU_K = 0.044715

STEPS = 3
LAYERS = 2
BATCH = 1024
DM = 256
DF = 1024
FB = 256
NB = DF // FB
RT = 256
NR = BATCH // RT
RT1 = 256
MESH = pl.DeviceIdType.MESH
F32 = jnp.float32
BF16 = jnp.bfloat16

EARLY = 2
SEND_ORDER = [(1, b) for b in range(EARLY)] + [(0, b) for b in range(NB)] + [(1, b) for b in range(EARLY, NB)]


def dot_nn(a, b):
    return lax.dot_general(a, b, (((1,), (0,)), ((), ())), preferred_element_type=F32)


def dot_nt(a, b):
    return lax.dot_general(a, b, (((1,), (1,)), ((), ())), preferred_element_type=F32)


def dot_tn(a, b):
    return lax.dot_general(a, b, (((0,), (0,)), ((), ())), preferred_element_type=F32)


def kernel(n_rows, n_cols, w1_hbm, w2_hbm, a_hbm, t_hbm, wgt,
           wlo, wire, recv, ain, tin, nlo, nf1, inv1, act, acc, err, elo, dzb, macc,
           load_sem, data_sem, send_sem, recv_sem, relay_sem):
    row = lax.axis_index("row")
    col = lax.axis_index("col")
    half = row // 2
    inner = jnp.logical_and(row > 0, row < n_rows - 1)
    targets = (
        ((row, lax.rem(col + 1, n_cols)), 0),
        ((row, lax.rem(col + n_cols - 1, n_cols)), 1),
        ((row + 1 - 2 * half, col), lax.rem(row + half, 2) * -1 + 3),
        ((row - 1 + 2 * half, col), 2),
    )
    relay_device = (3 - 3 * half, col)

    def load_one(layer, blk):
        return pltpu.make_async_copy(
            w1_hbm.at[layer, :, pl.ds(pl.multiple_of(blk * FB, FB), FB)], wgt.at[layer, blk, 0], load_sem.at[layer, blk])

    def load_two(layer, blk):
        return pltpu.make_async_copy(
            w2_hbm.at[layer, pl.ds(pl.multiple_of(blk * FB, FB), FB), :], wgt.at[layer, blk, 1], load_sem.at[layer, blk])

    def loaded(layer, blk):
        return pltpu.make_async_copy(wgt.at[layer, blk], wgt.at[layer, blk], load_sem.at[layer, blk])

    def load_data(which, first, count):
        src, dst = ((a_hbm, ain), (t_hbm, tin))[which]
        return pltpu.make_async_copy(src.at[pl.ds(first, count)], dst.at[pl.ds(first, count)], data_sem.at[which, min(first, 1)])

    load_data(0, 0, 1).start()

    @pl.loop(0, LAYERS * NB)
    def _(i):
        load_one(i // NB, lax.rem(i, NB)).start()
        load_two(i // NB, lax.rem(i, NB)).start()

    barrier = pltpu.get_barrier_semaphore()
    for shift in range(1, n_rows):
        pl.semaphore_signal(barrier, inc=1, device_id=(lax.rem(row + shift, n_rows), col), device_id_type=MESH)
    for tgt, _ in targets[:2]:
        pl.semaphore_signal(barrier, inc=1, device_id=tgt, device_id_type=MESH)
    load_data(1, 0, 1).start()
    load_data(0, 1, STEPS - 1).start()
    load_data(1, 1, STEPS - 1).start()

    def remote(src, dst, sent, arrived, device):
        return pltpu.make_async_remote_copy(
            src_ref=src, dst_ref=dst, send_sem=sent, recv_sem=arrived, device_id=device, device_id_type=MESH)

    def send(step, kind, layer, *blk):
        device, slot = targets[kind]
        group = slot - 2 if kind == 2 else 0
        return remote(
            wire.at[(layer,) + blk], recv.at[(step, slot, layer) + blk],
            send_sem.at[kind], recv_sem.at[lax.rem(step, 2), group, layer, blk[0]], device)

    def relay(step, layer, blk):
        return remote(
            recv.at[step, 3, layer, blk], recv.at[step, 3, layer, blk],
            relay_sem.at[0], recv_sem.at[lax.rem(step, 2), 1, layer, blk], relay_device)

    def wait_far(step, layer, blk):
        relay(step, layer, blk).wait_recv()

    def wait_rest(step, layer, blk):
        dst = recv.at[step, pl.ds(0, 3), layer, blk]
        remote(dst, dst, send_sem.at[0], recv_sem.at[lax.rem(step, 2), 0, layer, blk], relay_device).wait_recv()

    def wait_relays(step):
        remote(recv.at[step, 3], recv.at[step, 3], relay_sem.at[0], recv_sem.at[0, 0, 0, 0], relay_device).wait_send()

    def start_sends(step, layer, *blk, hold=False):
        if hold:
            @pl.when(jnp.logical_not(jnp.logical_and(inner, step == STEPS - 1)))
            def _():
                send(step, 2, layer, *blk).start()
        else:
            send(step, 2, layer, *blk).start()

        @pl.when(jnp.logical_and(inner, step == 0))
        def _():
            send(step, 3, layer, *blk).start()
        for kind in (0, 1):
            send(step, kind, layer, *blk).start()

    def start_outward(step):
        @pl.when(jnp.logical_and(inner, step > 0))
        def _():
            wait_relays(step - 1)
            for layer, blk in SEND_ORDER:
                send(step, 3, layer, blk).start()

    def wait_sends():
        for kind in range(3):
            remote(wire, recv.at[0, 0], send_sem.at[kind], recv_sem.at[0, 0, 0, 0], relay_device).wait_send()

        @pl.when(inner)
        def _():
            remote(wire, recv.at[0, 0], send_sem.at[3], recv_sem.at[0, 0, 0, 0], relay_device).wait_send()

    def combine(step, layer, blk, keep_lo, held_back=False):
        with jax.named_scope("w_far"):
            wait_far(step, layer, blk)

        @pl.when(inner)
        def _():
            relay(step, layer, blk).start()
        if held_back:
            @pl.when(inner)
            def _():
                send(step, 2, layer, blk).start()
        with jax.named_scope("w_rest"):
            wait_rest(step, layer, blk)
        for which in range(2):
            @pl.loop(0, FB, step=64)
            def _(r0):
                rows = pl.ds(pl.multiple_of(r0, 64), 64)
                tot = wgt[layer, blk, which, rows]
                for slot in (0, 1, 3 - half, 2 + half):
                    tot = tot + recv[step, slot, layer, blk, which, rows].astype(F32)
                tot = tot * 0.2
                wgt[layer, blk, which, rows] = tot
                if keep_lo:
                    wlo[layer, blk, which, rows] = (tot if which else 0.5 * tot).astype(BF16)

    def normalise(layer, rows, x):
        inv = lax.rsqrt(jnp.mean(x * x, axis=-1, keepdims=True) + NORM_EPS)
        n = x * inv
        nlo[layer, rows] = n.astype(BF16)
        if layer == 1:
            nf1[rows] = n
            inv1[rows] = jnp.broadcast_to(inv, (x.shape[0], 128))

    def activation(layer, blk, rows):
        half_z = dot_nn(nlo[layer, rows], wlo[layer, blk, 0])
        th = jnp.tanh(half_z * (2.0 * GELU_C + (8.0 * GELU_C * GELU_K) * (half_z * half_z)))
        act[layer, blk, rows] = (half_z * (1.0 + th)).astype(BF16)
        return act[layer, blk, rows]

    def error(step, rows, total):
        e = (2.0 / (BATCH * DM)) * (total.astype(BF16).astype(F32) - tin[step, rows].astype(F32))
        err[rows] = e
        elo[rows] = e.astype(BF16)

    def first_forward():
        load_data(0, 0, 1).wait()
        for layer in range(LAYERS):
            if layer == LAYERS - 1:
                load_data(1, 0, 1).wait()
            for r in range(BATCH // RT1):
                rows = pl.ds(r * RT1, RT1)
                if layer == 0:
                    total = ain[0, rows].astype(F32)
                    normalise(layer, rows, total)
                else:
                    total = acc[rows]
                for blk in range(NB):
                    if r == 0:
                        loaded(layer, blk).wait()
                        wlo[layer, blk, 0] = (0.5 * wgt[layer, blk, 0]).astype(BF16)
                        wlo[layer, blk, 1] = wgt[layer, blk, 1].astype(BF16)
                    total = total + dot_nn(activation(layer, blk, rows), wlo[layer, blk, 1])
                if layer == 0:
                    total = total.astype(BF16).astype(F32)
                    normalise(1, rows, total)
                    acc[rows] = total
                else:
                    error(0, rows, total)

    def forward_layer(step, layer):
        for r0 in range(0, BATCH, 128):
            rows = pl.ds(r0, 128)
            x = ain[step, rows].astype(F32) if layer == 0 else acc[rows].astype(BF16).astype(F32)
            normalise(layer, rows, x)
            acc[rows] = x

        @pl.loop(0, NB)
        def _(blk):
            combine(step - 1, layer, blk, True)
            for r in range(NR):
                rows = pl.ds(r * RT, RT)
                acc[rows] = acc[rows] + dot_nn(activation(layer, blk, rows), wlo[layer, blk, 1])

    def backward_layer(step, layer, send_now):
        if layer > 0:
            @pl.loop(0, BATCH, step=128)
            def _(r0):
                rows = pl.ds(pl.multiple_of(r0, 128), 128)
                macc[rows] = jnp.zeros((128, DM), F32)

        @pl.loop(0, NB)
        def _(blk):
            g_two = dot_tn(act[layer, blk], elo[...])
            q_two = wgt[layer, blk, 1] - LEARN_RATE * g_two
            wgt[layer, blk, 1] = q_two
            wire[layer, blk, 1] = q_two.astype(BF16)
            send_now(blk, 1)
            w_one = wlo[layer, blk, 0]
            w_two = wlo[layer, blk, 1]
            for r in range(NR):
                rows = pl.ds(r * RT, RT)
                u = dot_nt(elo[rows], w_two)
                half_z = dot_nn(nlo[layer, rows], w_one)
                sq = half_z * half_z
                th = jnp.tanh(half_z * (2.0 * GELU_C + (8.0 * GELU_C * GELU_K) * sq))
                slope = (0.5 + 0.5 * th) * (1.0 + (half_z * (1.0 - th)) * (2.0 * GELU_C + (24.0 * GELU_C * GELU_K) * sq))
                dz = (u * slope).astype(BF16)
                dzb[rows] = dz
                if layer > 0:
                    macc[rows] = macc[rows] + dot_nt(dz, w_one)
            g_one = dot_tn(nlo[layer], dzb[...])
            q_one = wgt[layer, blk, 0] - LEARN_RATE * g_one
            wgt[layer, blk, 0] = q_one
            wire[layer, blk, 0] = q_one.astype(BF16)
            send_now(blk, 0)

    with jax.named_scope("fwd_first"):
        first_forward()
    pl.semaphore_wait(barrier, n_rows + 1)

    @pl.loop(0, STEPS)
    def _(step):
        @pl.when(step > 0)
        def _():
            wait_sends()

        def send_early(blk, which):
            @pl.when(blk < EARLY)
            def _():
                start_sends(step, 1, blk, which)

        with jax.named_scope("bwd1"):
            backward_layer(step, 1, send_early)

        @pl.loop(0, BATCH, step=128)
        def _(r0):
            rows = pl.ds(pl.multiple_of(r0, 128), 128)
            m = 2.0 * macc[rows]
            n = nf1[rows]
            inv = inv1[rows, 0:1]
            e = err[rows] + inv * (m - n * jnp.mean(m * n, axis=-1, keepdims=True))
            elo[rows] = e.astype(BF16)

        def send_whole(blk, which):
            if which == 0:
                start_sends(step, 0, blk)

        with jax.named_scope("bwd0"):
            backward_layer(step, 0, send_whole)
        for blk in range(EARLY, NB):
            start_sends(step, 1, blk, hold=(1, blk) == SEND_ORDER[-1])
        with jax.named_scope("outward"):
            start_outward(step)

        @pl.when(step == 0)
        def _():
            load_data(0, 1, STEPS - 1).wait()
            load_data(1, 1, STEPS - 1).wait()

        @pl.when(step < STEPS - 1)
        def _():
            with jax.named_scope("fwd0"):
                forward_layer(step + 1, 0)
            with jax.named_scope("fwd1"):
                forward_layer(step + 1, 1)
            for r0 in range(0, BATCH, 128):
                error(step + 1, pl.ds(r0, 128), acc[pl.ds(r0, 128)])

    for layer, blk in SEND_ORDER:
        combine(STEPS - 1, layer, blk, False, held_back=(layer, blk) == SEND_ORDER[-1])
    wait_sends()

    @pl.when(inner)
    def _():
        wait_relays(STEPS - 1)


def store_kernel(wgt, o1_hbm, o2_hbm, out_sem):
    copies = []
    for layer in range(LAYERS):
        for blk in range(NB):
            span = pl.ds(blk * FB, FB)
            copies.append(pltpu.make_async_copy(wgt.at[layer, blk, 0], o1_hbm.at[layer, :, span], out_sem.at[layer, blk, 0]))
            copies.append(pltpu.make_async_copy(wgt.at[layer, blk, 1], o2_hbm.at[layer, span, :], out_sem.at[layer, blk, 1]))
    for copy in copies:
        copy.start()
    for copy in copies:
        copy.wait()


def solution(mesh):
    n_rows = mesh.shape["row"]
    n_cols = mesh.shape["col"]

    def device_fn(w_one, w_two, inputs, targets):
        chunk = (LAYERS, NB, 2, FB, DM)
        weights = pl.pallas_call(
            functools.partial(kernel, n_rows, n_cols),
            out_shape=pltpu.VMEM(chunk, F32),
            in_specs=[pl.BlockSpec(memory_space=pl.ANY)] * 4,
            out_specs=pl.BlockSpec(memory_space=pltpu.VMEM),
            scratch_shapes=[
                pltpu.VMEM(chunk, BF16),
                pltpu.VMEM(chunk, BF16),
                pltpu.VMEM((STEPS, 4) + chunk, BF16),
                pltpu.VMEM((STEPS, BATCH, DM), BF16),
                pltpu.VMEM((STEPS, BATCH, DM), BF16),
                pltpu.VMEM((LAYERS, BATCH, DM), BF16),
                pltpu.VMEM((BATCH, DM), F32),
                pltpu.VMEM((BATCH, 128), F32),
                pltpu.VMEM((LAYERS, NB, BATCH, FB), BF16),
                pltpu.VMEM((BATCH, DM), F32),
                pltpu.VMEM((BATCH, DM), F32),
                pltpu.VMEM((BATCH, DM), BF16),
                pltpu.VMEM((BATCH, FB), BF16),
                pltpu.VMEM((BATCH, DM), F32),
                pltpu.SemaphoreType.DMA((LAYERS, NB)),
                pltpu.SemaphoreType.DMA((2, 2)),
                pltpu.SemaphoreType.DMA((4,)),
                pltpu.SemaphoreType.DMA((2, 2, LAYERS, NB)),
                pltpu.SemaphoreType.DMA((1,)),
            ],
            compiler_params=pltpu.CompilerParams(
                collective_id=0, has_side_effects=True, vmem_limit_bytes=58 * 2**20),
        )(w_one[0, 0], w_two[0, 0], inputs[0, 0], targets[0, 0])
        out_one, out_two = pl.pallas_call(
            store_kernel,
            out_shape=[
                jax.ShapeDtypeStruct((LAYERS, DM, DF), F32),
                jax.ShapeDtypeStruct((LAYERS, DF, DM), F32),
            ],
            in_specs=[pl.BlockSpec(memory_space=pltpu.VMEM)],
            out_specs=[pl.BlockSpec(memory_space=pl.ANY)] * 2,
            scratch_shapes=[pltpu.SemaphoreType.DMA((LAYERS, NB, 2))],
            compiler_params=pltpu.CompilerParams(vmem_limit_bytes=2**20),
        )(weights)
        return out_one[None, None], out_two[None, None]

    grid_spec = P("row", "col")
    return jax.shard_map(device_fn, mesh=mesh, in_specs=(grid_spec,) * 4, out_specs=(grid_spec,) * 2, check_vma=False)
```

```python
import functools

import jax
import jax.numpy as jnp
from jax import lax
from jax.experimental import pallas as pl
from jax.experimental.pallas import tpu as pltpu
from jax.sharding import PartitionSpec as P

LEARN_RATE = 1.5
NORM_EPS = 1e-6
GELU_C = 0.7978845608028654
GELU_K = 0.044715

STEPS = 3
LAYERS = 2
BATCH = 1024
DM = 256
DF = 1024
FB = 256
NB = DF // FB
RT = 256
NR = BATCH // RT
RT1 = 512
MESH = pl.DeviceIdType.MESH
F32 = jnp.float32
BF16 = jnp.bfloat16

EARLY = 2
SEND_ORDER = [(1, b) for b in range(EARLY)] + [(0, b) for b in range(NB)] + [(1, b) for b in range(EARLY, NB)]


def dot_nn(a, b):
    return lax.dot_general(a, b, (((1,), (0,)), ((), ())), preferred_element_type=F32)


def dot_nt(a, b):
    return lax.dot_general(a, b, (((1,), (1,)), ((), ())), preferred_element_type=F32)


def dot_tn(a, b):
    return lax.dot_general(a, b, (((0,), (0,)), ((), ())), preferred_element_type=F32)


def kernel(n_rows, n_cols, w1_hbm, w2_hbm, a_hbm, t_hbm, wgt,
           wlo, wire, recv, ain, tin, nlo, nf1, inv1, act, acc, err, elo, dzb, macc,
           load_sem, data_sem, send_sem, recv_sem, relay_sem):
    row = lax.axis_index("row")
    col = lax.axis_index("col")
    half = row // 2
    inner = jnp.logical_and(row > 0, row < n_rows - 1)
    targets = (
        ((row, lax.rem(col + 1, n_cols)), 0),
        ((row, lax.rem(col + n_cols - 1, n_cols)), 1),
        ((row + 1 - 2 * half, col), lax.rem(row + half, 2) * -1 + 3),
        ((row - 1 + 2 * half, col), 2),
    )
    relay_device = (3 - 3 * half, col)

    def load_one(layer, blk):
        return pltpu.make_async_copy(
            w1_hbm.at[layer, :, pl.ds(pl.multiple_of(blk * FB, FB), FB)], wgt.at[layer, blk, 0], load_sem.at[layer, blk])

    def load_two(layer, blk):
        return pltpu.make_async_copy(
            w2_hbm.at[layer, pl.ds(pl.multiple_of(blk * FB, FB), FB), :], wgt.at[layer, blk, 1], load_sem.at[layer, blk])

    def loaded(layer, blk):
        return pltpu.make_async_copy(wgt.at[layer, blk], wgt.at[layer, blk], load_sem.at[layer, blk])

    def load_data(which, first, count):
        src, dst = ((a_hbm, ain), (t_hbm, tin))[which]
        return pltpu.make_async_copy(src.at[pl.ds(first, count)], dst.at[pl.ds(first, count)], data_sem.at[which, min(first, 1)])

    load_data(0, 0, 1).start()

    @pl.loop(0, LAYERS * NB)
    def _(i):
        load_one(i // NB, lax.rem(i, NB)).start()
        load_two(i // NB, lax.rem(i, NB)).start()

    barrier = pltpu.get_barrier_semaphore()
    for shift in range(1, n_rows):
        pl.semaphore_signal(barrier, inc=1, device_id=(lax.rem(row + shift, n_rows), col), device_id_type=MESH)
    for tgt, _ in targets[:2]:
        pl.semaphore_signal(barrier, inc=1, device_id=tgt, device_id_type=MESH)
    load_data(1, 0, 1).start()
    load_data(0, 1, STEPS - 1).start()
    load_data(1, 1, STEPS - 1).start()

    def remote(src, dst, sent, arrived, device):
        return pltpu.make_async_remote_copy(
            src_ref=src, dst_ref=dst, send_sem=sent, recv_sem=arrived, device_id=device, device_id_type=MESH)

    def send(step, kind, layer, *blk):
        device, slot = targets[kind]
        group = slot - 2 if kind == 2 else 0
        return remote(
            wire.at[(layer,) + blk], recv.at[(step, slot, layer) + blk],
            send_sem.at[kind], recv_sem.at[lax.rem(step, 2), group, layer, blk[0]], device)

    def relay(step, layer, blk):
        return remote(
            recv.at[step, 3, layer, blk], recv.at[step, 3, layer, blk],
            relay_sem.at[0], recv_sem.at[lax.rem(step, 2), 1, layer, blk], relay_device)

    def wait_far(step, layer, blk):
        relay(step, layer, blk).wait_recv()

    def wait_rest(step, layer, blk):
        dst = recv.at[step, pl.ds(0, 3), layer, blk]
        remote(dst, dst, send_sem.at[0], recv_sem.at[lax.rem(step, 2), 0, layer, blk], relay_device).wait_recv()

    def wait_relays(step):
        remote(recv.at[step, 3], recv.at[step, 3], relay_sem.at[0], recv_sem.at[0, 0, 0, 0], relay_device).wait_send()

    def start_sends(step, layer, *blk, hold=False):
        if hold:
            @pl.when(jnp.logical_not(jnp.logical_and(inner, step == STEPS - 1)))
            def _():
                send(step, 2, layer, *blk).start()
        else:
            send(step, 2, layer, *blk).start()

        @pl.when(jnp.logical_and(inner, step == 0))
        def _():
            send(step, 3, layer, *blk).start()
        for kind in (0, 1):
            send(step, kind, layer, *blk).start()

    def start_outward(step):
        @pl.when(jnp.logical_and(inner, step > 0))
        def _():
            wait_relays(step - 1)
            for layer, blk in SEND_ORDER:
                send(step, 3, layer, blk).start()

    def wait_sends():
        for kind in range(3):
            remote(wire, recv.at[0, 0], send_sem.at[kind], recv_sem.at[0, 0, 0, 0], relay_device).wait_send()

        @pl.when(inner)
        def _():
            remote(wire, recv.at[0, 0], send_sem.at[3], recv_sem.at[0, 0, 0, 0], relay_device).wait_send()

    def combine(step, layer, blk, keep_lo, held_back=False):
        with jax.named_scope("w_far"):
            wait_far(step, layer, blk)

        @pl.when(inner)
        def _():
            relay(step, layer, blk).start()
        if held_back:
            @pl.when(inner)
            def _():
                send(step, 2, layer, blk).start()
        with jax.named_scope("w_rest"):
            wait_rest(step, layer, blk)
        for which in range(2):
            @pl.loop(0, FB, step=64)
            def _(r0):
                rows = pl.ds(pl.multiple_of(r0, 64), 64)
                tot = wgt[layer, blk, which, rows]
                for slot in (0, 1, 3 - half, 2 + half):
                    tot = tot + recv[step, slot, layer, blk, which, rows].astype(F32)
                tot = tot * 0.2
                wgt[layer, blk, which, rows] = tot
                if keep_lo:
                    wlo[layer, blk, which, rows] = (tot if which else 0.5 * tot).astype(BF16)

    def normalise(layer, rows, x):
        inv = lax.rsqrt(jnp.mean(x * x, axis=-1, keepdims=True) + NORM_EPS)
        n = x * inv
        nlo[layer, rows] = n.astype(BF16)
        if layer == 1:
            nf1[rows] = n
            inv1[rows] = jnp.broadcast_to(inv, (x.shape[0], 128))

    def activation(layer, blk, rows):
        half_z = dot_nn(nlo[layer, rows], wlo[layer, blk, 0])
        th = jnp.tanh(half_z * (2.0 * GELU_C + (8.0 * GELU_C * GELU_K) * (half_z * half_z)))
        act[layer, blk, rows] = (half_z * (1.0 + th)).astype(BF16)
        return act[layer, blk, rows]

    def error(step, rows, total):
        e = (2.0 / (BATCH * DM)) * (total.astype(BF16).astype(F32) - tin[step, rows].astype(F32))
        err[rows] = e
        elo[rows] = e.astype(BF16)

    def first_forward():
        load_data(0, 0, 1).wait()
        for layer in range(LAYERS):
            if layer == LAYERS - 1:
                load_data(1, 0, 1).wait()
            if layer == 0:
                for r0 in range(0, BATCH, 128):
                    rows = pl.ds(r0, 128)
                    normalise(layer, rows, ain[0, rows].astype(F32))
            for blk in range(NB):
                loaded(layer, blk).wait()
            for blk in range(NB):
                wlo[layer, blk, 0] = (0.5 * wgt[layer, blk, 0]).astype(BF16)
                wlo[layer, blk, 1] = wgt[layer, blk, 1].astype(BF16)
            for r in range(BATCH // RT1):
                rows = pl.ds(r * RT1, RT1)
                if layer == 0:
                    total = ain[0, rows].astype(F32)
                else:
                    total = acc[rows]
                for blk in range(NB):
                    total = total + dot_nn(activation(layer, blk, rows), wlo[layer, blk, 1])
                if layer == 0:
                    total = total.astype(BF16).astype(F32)
                    normalise(1, rows, total)
                    acc[rows] = total
                else:
                    error(0, rows, total)

    def forward_layer(step, layer):
        for r0 in range(0, BATCH, 128):
            rows = pl.ds(r0, 128)
            x = ain[step, rows].astype(F32) if layer == 0 else acc[rows].astype(BF16).astype(F32)
            normalise(layer, rows, x)
            acc[rows] = x

        @pl.loop(0, NB)
        def _(blk):
            combine(step - 1, layer, blk, True)
            for r in range(NR):
                rows = pl.ds(r * RT, RT)
                acc[rows] = acc[rows] + dot_nn(activation(layer, blk, rows), wlo[layer, blk, 1])

    def backward_layer(step, layer, send_now):
        if layer > 0:
            @pl.loop(0, BATCH, step=128)
            def _(r0):
                rows = pl.ds(pl.multiple_of(r0, 128), 128)
                macc[rows] = jnp.zeros((128, DM), F32)

        @pl.loop(0, NB)
        def _(blk):
            g_two = dot_tn(act[layer, blk], elo[...])
            q_two = wgt[layer, blk, 1] - LEARN_RATE * g_two
            wgt[layer, blk, 1] = q_two
            wire[layer, blk, 1] = q_two.astype(BF16)
            send_now(blk, 1)
            w_one = wlo[layer, blk, 0]
            w_two = wlo[layer, blk, 1]
            for r in range(NR):
                rows = pl.ds(r * RT, RT)
                u = dot_nt(elo[rows], w_two)
                half_z = dot_nn(nlo[layer, rows], w_one)
                sq = half_z * half_z
                th = jnp.tanh(half_z * (2.0 * GELU_C + (8.0 * GELU_C * GELU_K) * sq))
                slope = (0.5 + 0.5 * th) * (1.0 + (half_z * (1.0 - th)) * (2.0 * GELU_C + (24.0 * GELU_C * GELU_K) * sq))
                dz = (u * slope).astype(BF16)
                dzb[rows] = dz
                if layer > 0:
                    macc[rows] = macc[rows] + dot_nt(dz, w_one)
            g_one = dot_tn(nlo[layer], dzb[...])
            q_one = wgt[layer, blk, 0] - LEARN_RATE * g_one
            wgt[layer, blk, 0] = q_one
            wire[layer, blk, 0] = q_one.astype(BF16)
            send_now(blk, 0)

    with jax.named_scope("fwd_first"):
        first_forward()
    pl.semaphore_wait(barrier, n_rows + 1)

    @pl.loop(0, STEPS)
    def _(step):
        @pl.when(step > 0)
        def _():
            wait_sends()

        def send_early(blk, which):
            @pl.when(blk < EARLY)
            def _():
                start_sends(step, 1, blk, which)

        with jax.named_scope("bwd1"):
            backward_layer(step, 1, send_early)

        @pl.loop(0, BATCH, step=128)
        def _(r0):
            rows = pl.ds(pl.multiple_of(r0, 128), 128)
            m = 2.0 * macc[rows]
            n = nf1[rows]
            inv = inv1[rows, 0:1]
            e = err[rows] + inv * (m - n * jnp.mean(m * n, axis=-1, keepdims=True))
            elo[rows] = e.astype(BF16)

        def send_whole(blk, which):
            if which == 0:
                start_sends(step, 0, blk)

        with jax.named_scope("bwd0"):
            backward_layer(step, 0, send_whole)
        for blk in range(EARLY, NB):
            start_sends(step, 1, blk, hold=(1, blk) == SEND_ORDER[-1])
        with jax.named_scope("outward"):
            start_outward(step)

        @pl.when(step == 0)
        def _():
            load_data(0, 1, STEPS - 1).wait()
            load_data(1, 1, STEPS - 1).wait()

        @pl.when(step < STEPS - 1)
        def _():
            with jax.named_scope("fwd0"):
                forward_layer(step + 1, 0)
            with jax.named_scope("fwd1"):
                forward_layer(step + 1, 1)
            for r0 in range(0, BATCH, 128):
                error(step + 1, pl.ds(r0, 128), acc[pl.ds(r0, 128)])

    for layer, blk in SEND_ORDER:
        combine(STEPS - 1, layer, blk, False, held_back=(layer, blk) == SEND_ORDER[-1])
    wait_sends()

    @pl.when(inner)
    def _():
        wait_relays(STEPS - 1)


def store_kernel(wgt, o1_hbm, o2_hbm, out_sem):
    copies = []
    for layer in range(LAYERS):
        for blk in range(NB):
            span = pl.ds(blk * FB, FB)
            copies.append(pltpu.make_async_copy(wgt.at[layer, blk, 0], o1_hbm.at[layer, :, span], out_sem.at[layer, blk, 0]))
            copies.append(pltpu.make_async_copy(wgt.at[layer, blk, 1], o2_hbm.at[layer, span, :], out_sem.at[layer, blk, 1]))
    for copy in copies:
        copy.start()
    for copy in copies:
        copy.wait()


def solution(mesh):
    n_rows = mesh.shape["row"]
    n_cols = mesh.shape["col"]

    def device_fn(w_one, w_two, inputs, targets):
        chunk = (LAYERS, NB, 2, FB, DM)
        weights = pl.pallas_call(
            functools.partial(kernel, n_rows, n_cols),
            out_shape=pltpu.VMEM(chunk, F32),
            in_specs=[pl.BlockSpec(memory_space=pl.ANY)] * 4,
            out_specs=pl.BlockSpec(memory_space=pltpu.VMEM),
            scratch_shapes=[
                pltpu.VMEM(chunk, BF16),
                pltpu.VMEM(chunk, BF16),
                pltpu.VMEM((STEPS, 4) + chunk, BF16),
                pltpu.VMEM((STEPS, BATCH, DM), BF16),
                pltpu.VMEM((STEPS, BATCH, DM), BF16),
                pltpu.VMEM((LAYERS, BATCH, DM), BF16),
                pltpu.VMEM((BATCH, DM), F32),
                pltpu.VMEM((BATCH, 128), F32),
                pltpu.VMEM((LAYERS, NB, BATCH, FB), BF16),
                pltpu.VMEM((BATCH, DM), F32),
                pltpu.VMEM((BATCH, DM), F32),
                pltpu.VMEM((BATCH, DM), BF16),
                pltpu.VMEM((BATCH, FB), BF16),
                pltpu.VMEM((BATCH, DM), F32),
                pltpu.SemaphoreType.DMA((LAYERS, NB)),
                pltpu.SemaphoreType.DMA((2, 2)),
                pltpu.SemaphoreType.DMA((4,)),
                pltpu.SemaphoreType.DMA((2, 2, LAYERS, NB)),
                pltpu.SemaphoreType.DMA((1,)),
            ],
            compiler_params=pltpu.CompilerParams(
                collective_id=0, has_side_effects=True, vmem_limit_bytes=58 * 2**20),
        )(w_one[0, 0], w_two[0, 0], inputs[0, 0], targets[0, 0])
        out_one, out_two = pl.pallas_call(
            store_kernel,
            out_shape=[
                jax.ShapeDtypeStruct((LAYERS, DM, DF), F32),
                jax.ShapeDtypeStruct((LAYERS, DF, DM), F32),
            ],
            in_specs=[pl.BlockSpec(memory_space=pltpu.VMEM)],
            out_specs=[pl.BlockSpec(memory_space=pl.ANY)] * 2,
            scratch_shapes=[pltpu.SemaphoreType.DMA((LAYERS, NB, 2))],
            compiler_params=pltpu.CompilerParams(vmem_limit_bytes=2**20),
        )(weights)
        return out_one[None, None], out_two[None, None]

    grid_spec = P("row", "col")
    return jax.shard_map(device_fn, mesh=mesh, in_specs=(grid_spec,) * 4, out_specs=(grid_spec,) * 2, check_vma=False)
```
